32 devices in a mesh: vox: 8 (over y, x, core), sen: 4 (over z).
Axes of the slice: x: 2, y: 2, z: 4, core: 2. Of those that a mesh axis runs over, the one named last changes fastest.
Arguments:
- image: float32 [8, 2, 512], P('vox'), may hold values from -6 to 6
- weights: bfloat16 [8, 4, 5, 1024, 1024], P('vox', 'sen'), may hold values from -0.0625 to 0.0625
- block_ids: int32 [8, 4, 5], P('vox', 'sen'), may hold values from 0 to 15
- offsets: int32 [8, 4, 5], P('vox', 'sen'), may hold values from 0 to 1984
- counts: int32 [8, 4], P('vox', 'sen'), may hold values from 1 to 5, as said below
- measured: bfloat16 [4, 256, 2048], P('sen', 'vox'), may hold values from -6 to 6
Outputs:
- image_next: float32 [8, 2, 512], P('vox')
- residual: float32 [4, 256, 2048], P('sen', 'vox')
The draws below stay inside these ranges and needn't reach their ends.
Inputs may be any that keep to these rules, and one draw needn't show every extreme that they name: `counts`: some slab and group has all 5 slots live in every draw.
All inputs are finite; a program needn't handle non-finite values.
Results may differ from the reference program's by a relative error of at most 0.0025.
Values may be sent and summed in bfloat16 or wider, within the bound.
A program may use at most 64 MiB of HBM per device.

```python
import jax
import jax.numpy as jnp
from jax import lax

SAMPLES = 2048
SB = 16
WIN = 64
K_MAX = 5
ZS = 1
PY = 2
PX = 512
SLABS = 8
GROUPS = 4
GSENS = 256
BLOCKS = 16
NZ = 8


def draw_counts(key, part):
    first_key, second_key = jax.random.split(jax.random.fold_in(key, 17))
    drawn_counts = jax.random.randint(first_key, (SLABS, GROUPS), 1, K_MAX + 1)
    chosen = jax.random.randint(second_key, (), 0, SLABS * GROUPS)
    flat_index = jnp.arange(SLABS * GROUPS).reshape(SLABS, GROUPS)
    return jnp.where(flat_index == chosen, K_MAX, drawn_counts).astype(jnp.int32)


def touch_ends(drawn, key, least, largest):
    shape = drawn.shape
    spot = [jax.random.randint(jax.random.fold_in(key, axis), (), 0, shape[axis]) for axis in range(len(shape))]
    drawn = drawn.at[tuple(spot)].set(least)
    longest = shape.index(max(shape))
    spot[longest] = (spot[longest] + 1) % shape[longest]
    return drawn.at[tuple(spot)].set(largest)


def steps_of(rng, extent, cuts, low, high):
    gain, own = 1.0, jax.random.fold_in(rng, 6)
    for dim, blocks in cuts:
        draws = jnp.exp(jax.random.uniform(jax.random.fold_in(own, dim), (blocks,), jnp.float32, low / len(cuts), high / len(cuts)))
        gain = gain * jnp.repeat(draws, extent[dim] // blocks).reshape([-1 if axis == dim else 1 for axis in range(len(extent))])
    return gain


def normal_values(rng, shape, width, limit, cuts=(), held_as=jnp.bfloat16):
    loudness = steps_of(rng, shape, cuts, -0.22, 0.18) if cuts else 1.0
    array = jax.random.normal(rng, shape, jnp.float32) * width * loudness
    return jnp.minimum(jnp.maximum(array, -limit), limit).astype(held_as)


def setup_inputs(seed: int = 0) -> dict:
    arg_keys = jax.random.split(jax.random.key(seed), 7)
    return {
        "image": normal_values(arg_keys[0], (NZ, PY, PX), 1.0, 6.0, ((0, 8),), jnp.float32),
        "weights": normal_values(arg_keys[1], (SLABS, GROUPS, K_MAX, ZS * PY * PX, SB * WIN), (8 * SB * WIN) ** -0.5, 0.0625, ((0, 8), (1, 4))),
        "block_ids": touch_ends(jax.random.randint(arg_keys[2], (SLABS, GROUPS, K_MAX), 0, BLOCKS), jax.random.fold_in(arg_keys[2], 1), 0, BLOCKS - 1).astype(jnp.int32),
        "offsets": touch_ends(jax.random.randint(arg_keys[3], (SLABS, GROUPS, K_MAX), 0, SAMPLES - WIN + 1), jax.random.fold_in(arg_keys[3], 1), 0, SAMPLES - WIN).astype(jnp.int32),
        "counts": draw_counts(jax.random.fold_in(arg_keys[6], 71), 0),
        "measured": normal_values(arg_keys[5], (GROUPS, GSENS, SAMPLES), 1.0, 6.0, ((0, 4), (1, 8))),
    }


TAPS = ((-2, 1.0 / 12.0), (-1, -8.0 / 12.0), (1, 8.0 / 12.0), (2, -1.0 / 12.0))
STEP_SIZE = 0.25
TV_WEIGHT = 0.3
TV_EPS = 0.01

def derivative(signal):
    length_t = signal.shape[-1]
    padded = jnp.pad(signal, [(0, 0)] * (signal.ndim - 1) + [(2, 2)])
    summed = jnp.zeros_like(signal)
    for shift_by, coefficient in TAPS:
        summed = summed + coefficient * padded[..., 2 + shift_by:2 + shift_by + length_t]
    return summed

def forward_step(volume, axis_dim):
    length_a = volume.shape[axis_dim]
    ahead = jnp.concatenate([lax.slice_in_dim(volume, 1, length_a, axis=axis_dim), lax.slice_in_dim(volume, length_a - 1, length_a, axis=axis_dim)], axis=axis_dim)
    return ahead - volume

def backward_shift(field, axis_dim):
    length_a = field.shape[axis_dim]
    zero_row = jnp.zeros_like(lax.slice_in_dim(field, 0, 1, axis=axis_dim))
    return jnp.concatenate([zero_row, lax.slice_in_dim(field, 0, length_a - 1, axis=axis_dim)], axis=axis_dim)

def tv_gradient(volume):
    step_z = forward_step(volume, 0)
    step_y = forward_step(volume, 1)
    step_x = forward_step(volume, 2)
    magnitude = jnp.sqrt(step_z * step_z + step_y * step_y + step_x * step_x + TV_EPS)
    result = jnp.zeros_like(volume)
    for axis_dim, step_a in ((0, step_z), (1, step_y), (2, step_x)):
        unit_a = step_a / magnitude
        result = result + backward_shift(unit_a, axis_dim) - unit_a
    return result

def reference(image, weights, block_ids, offsets, counts, measured):
    voxels = image.astype(jnp.bfloat16).astype(jnp.float32).reshape(SLABS, ZS * PY * PX)
    slot_grid = jnp.arange(K_MAX, dtype=jnp.int32)

    def add_slab(signals, inputs):
        slab_voxels, slab_blocks, slab_ids, slab_starts, slab_counts = inputs
        pieces = jnp.einsum('v,gkvc->gkc', slab_voxels, slab_blocks.astype(jnp.float32))

        def place(flat_index, acc):
            group_index = (flat_index // K_MAX).astype(jnp.int32)
            slot_index = (flat_index % K_MAX).astype(jnp.int32)
            live_flag = (slot_index < slab_counts[group_index]).astype(jnp.float32)
            piece = pieces[group_index, slot_index].reshape(1, SB, WIN) * live_flag
            corner = (group_index, (slab_ids[group_index, slot_index] * SB).astype(jnp.int32), slab_starts[group_index, slot_index].astype(jnp.int32))
            current = lax.dynamic_slice(acc, corner, (1, SB, WIN))
            return lax.dynamic_update_slice(acc, current + piece, corner)
        signals = lax.fori_loop(0, GROUPS * K_MAX, place, signals)
        return (signals, None)
    zero_signals = jnp.zeros((GROUPS, GSENS, SAMPLES), jnp.float32)
    signals, _ = lax.scan(add_slab, zero_signals, (voxels, weights, block_ids, offsets, counts))
    residual = derivative(signals) - measured.astype(jnp.float32)
    adjoint = lax.optimization_barrier((-derivative(residual)).astype(jnp.bfloat16)).astype(jnp.float32)
    group_grid = jnp.broadcast_to(jnp.arange(GROUPS, dtype=jnp.int32)[:, None], (GROUPS, K_MAX))

    def cut_window(group_index, block_index, start):
        corner = (group_index, (block_index * SB).astype(jnp.int32), start.astype(jnp.int32))
        return lax.dynamic_slice(adjoint, corner, (1, SB, WIN)).reshape(SB * WIN)

    def back_slab(carry, inputs):
        slab_blocks, slab_ids, slab_starts, slab_counts = inputs
        windows = jax.vmap(jax.vmap(cut_window))(group_grid, slab_ids, slab_starts)
        live = (slot_grid[None, :] < slab_counts[:, None]).astype(jnp.float32)
        windows = windows * live[:, :, None]
        grad_slab = jnp.einsum('gkc,gkvc->v', windows, slab_blocks.astype(jnp.float32))
        return (carry, grad_slab)
    _, backprojected = lax.scan(back_slab, jnp.zeros((), jnp.float32), (weights, block_ids, offsets, counts))
    backprojected = backprojected.reshape(NZ, PY, PX)
    image_next = image - STEP_SIZE * (backprojected + TV_WEIGHT * tv_gradient(image))
    return (image_next, residual)
```

```python
import functools

import jax
import jax.numpy as jnp
from jax import lax
from jax.experimental import pallas as pl
from jax.experimental.pallas import tpu as pltpu
from jax.sharding import PartitionSpec as P

SB = 16
WIN = 64
LANES = 128
HALF = 8
FAR = 1 << 16
UNROLL = 8

STEP_SIZE = 0.25
TV_WEIGHT = 0.3
TV_EPS = 0.01
C1 = 8.0 / 12.0
C2 = 1.0 / 12.0
MESH = pl.DeviceIdType.MESH


def lane_iota(shape):
    return lax.broadcasted_iota(jnp.int32, shape, len(shape) - 1)


def ahead(value, shift):
    length = value.shape[-1]
    return pltpu.roll(value, (-shift) % length, value.ndim - 1)


def stencil(value):
    return C2 * ahead(value, -2) - C1 * ahead(value, -1) + C1 * ahead(value, 1) - C2 * ahead(value, 2)


def stencil_edges(value):
    length = value.shape[-1]
    at = lane_iota(value.shape)
    total = jnp.where(at >= 2, C2 * ahead(value, -2), 0.0)
    total = total - jnp.where(at >= 1, C1 * ahead(value, -1), 0.0)
    total = total + jnp.where(at < length - 1, C1 * ahead(value, 1), 0.0)
    return total - jnp.where(at < length - 2, C2 * ahead(value, 2), 0.0)


def block_mask(width):
    row = lax.broadcasted_iota(jnp.int32, (SB, width), 0)
    return lane_iota((SB, width)) // WIN == row


def each(count, body, carry):
    if count > UNROLL:
        return lax.fori_loop(0, count, body, carry)
    for i in range(count):
        carry = body(i, carry)
    return carry


def gather_kernel(
    n, slots, chunks, image_in, weights, ids_in, offs_in, count, measured_in,
    turned, target, windows, halo, wbuf, image, measured,
    ids, offs, mine, meta, table, pieces_all, tiled, cuts, cuts_all,
    wsem, load_sem, local_sem, small_send, small_recv, halo_send, halo_recv,
    piece_send, piece_recv, cut_send, cut_recv,
):
    me = lax.axis_index("vox")
    voxels = weights.shape[3]
    depth = voxels // chunks
    rows, samples = measured.shape[1:]
    tiles = samples // LANES
    lines = min(rows, SB)
    parts = SB // lines
    per = max(rows // SB, 1)

    barrier = pltpu.get_barrier_semaphore()
    for step in range(1, n):
        pl.semaphore_signal(barrier, inc=1, device_id={"vox": (me + step) % n}, device_id_type=MESH)

    arguments = []
    pairs = ((ids_in, ids), (offs_in, offs), (image_in, image), (measured_in, measured))
    for i, (src, dst) in enumerate(pairs):
        load = pltpu.make_async_copy(src, dst, load_sem.at[i])
        load.start()
        arguments.append(load)
    loads = []
    for k in range(slots):
        for q in range(chunks):
            part = pl.ds(q * depth, depth)
            load = pltpu.make_async_copy(weights.at[0, 0, k, part], wbuf.at[k, part], wsem.at[k, q])
            load.start()
            loads.append(load)

    for load in arguments:
        load.wait()
    meta[...] = jnp.where(lane_iota(meta.shape) == slots, jnp.full(meta.shape, count[0, 0]), 0)
    meta[0:1, 0:slots] = ids[0]
    meta[1:2, 0:slots] = offs[0]
    for i in range(per * tiles):
        tiled[i] = measured[0, i // tiles * SB : i // tiles * SB + lines, i % tiles * LANES : (i % tiles + 1) * LANES]
    low = image[0].astype(jnp.bfloat16)
    flat = jnp.concatenate([low[r : r + 1] for r in range(low.shape[0])], axis=1)
    flat = jnp.broadcast_to(flat, (SB, voxels))
    mask = block_mask(SB * WIN)
    alive = jnp.full((SB, LANES), count[0, 0])
    left = lane_iota((SB, LANES)) < WIN
    pl.semaphore_wait(barrier, n - 1)

    def remote(src, dst, send, recv, target):
        return pltpu.make_async_remote_copy(
            src_ref=src, dst_ref=dst, send_sem=send, recv_sem=recv,
            device_id={"vox": target}, device_id_type=MESH,
        )

    small, sends, locals_ = [], [], []
    for step in range(1, n):
        copy = remote(meta, table.at[me], small_send.at[step], small_recv.at[step], (me + step) % n)
        copy.start()
        small.append(copy)
    own_meta = pltpu.make_async_copy(meta, table.at[me], local_sem.at[0])
    own_meta.start()
    for side, to in ((0, (me + 1) % n), (1, (me + n - 1) % n)):
        copy = remote(image.at[0], halo.at[side], halo_send.at[side], halo_recv.at[side], to)
        copy.start()
        sends.append(copy)

    at = lane_iota((HALF, LANES))

    def forward(k):
        total = jnp.zeros((SB, SB * WIN), jnp.float32)
        for q in range(chunks):
            loads[k * chunks + q].wait()
            total = total + jnp.dot(
                flat[:, q * depth : (q + 1) * depth],
                wbuf[k, q * depth : (q + 1) * depth],
                preferred_element_type=jnp.float32,
            )
        total = jnp.where(mask, total, 0.0)
        tile = total[:, 0:LANES]
        for g in range(1, SB * WIN // LANES):
            tile = tile + total[:, g * LANES : (g + 1) * LANES]
        tile = tile + pltpu.roll(tile, WIN, 1)
        return jnp.where(alive > k, tile, 0.0)

    def cut(j, carry):
        across = lane_iota((lines, LANES))
        for k in range(slots):
            near = jnp.clip(table[j, 0, k] - me * per, 0, per - 1) * tiles
            base = jnp.maximum(table[j, 1, k] - 2, 0)
            first = base // LANES
            after = jnp.minimum(first + 1, tiles - 1)
            edge = base % LANES
            one = tiled[near + first].astype(jnp.float32)
            two = tiled[near + after].astype(jnp.float32)
            both = jnp.where(across >= edge, one, two)
            cuts[j, k] = both.astype(cuts.dtype)
        return carry

    packed = None
    for k in range(slots):
        if k == slots - 1:
            own_meta.wait()
            for copy in small:
                copy.wait()
            each(n, cut, 0)
            exchanged = []
            for step in range(1, n):
                to = (me + step) % n
                copy = remote(cuts.at[to], cuts_all.at[me], cut_send.at[step], cut_recv.at[step], to)
                copy.start()
                exchanged.append(copy)
            copy = pltpu.make_async_copy(cuts.at[me], cuts_all.at[me], local_sem.at[1])
            copy.start()
            exchanged.append(copy)
        tile = forward(k)
        packed = jnp.where(left, tile, 0.0) if k % 2 == 0 else jnp.where(left, packed, tile)
        if k % 2 == 1 or k == slots - 1:
            g = k // 2
            mine[g] = packed
            group = []
            for step in range(1, n):
                copy = remote(
                    mine.at[g], pieces_all.at[me, g], piece_send.at[g, step], piece_recv.at[g, step],
                    (me + step) % n,
                )
                copy.start()
                group.append(copy)
            copy = pltpu.make_async_copy(mine.at[g], pieces_all.at[me, g], local_sem.at[2 + g])
            copy.start()
            group.append(copy)
            locals_.append(group)

    numbers = [table[me, 0, k] for k in range(slots)]
    starts = [table[me, 1, k] for k in range(slots)]
    times = [start - WIN // 2 + ((at - start + WIN // 2) & (LANES - 1)) for start in starts]
    keys = [number * FAR + time for number, time in zip(numbers, times)]
    lane = lane_iota((1, LANES))

    sums = [jnp.zeros((HALF, LANES), jnp.float32)] * (slots * 2)
    for g, group in enumerate(locals_):
        for copy in group:
            copy.wait()

        def gather(j, sums, g=g):
            sums = list(sums)
            packed = pieces_all[j, g]
            for k in range(2 * g, min(2 * g + 2, slots)):
                number, start = table[j, 0, k], table[j, 1, k]
                piece = pltpu.roll(packed, (start + (k % 2) * WIN) & (LANES - 1), 1)
                turned[j, k] = piece
                since = (lane - start) & (LANES - 1)
                spot = number * tiles + lax.shift_right_logical(since + start, 7)
                target[j, k : k + 1] = jnp.where(since < WIN, spot, -1)
                key = number * FAR + start
                for i in range(slots):
                    since = keys[i] - key
                    inside = (since >= 0) & (since < WIN)
                    for h in range(2):
                        part = piece[h * HALF : (h + 1) * HALF]
                        sums[2 * i + h] = sums[2 * i + h] + jnp.where(inside, part, 0.0)
            return tuple(sums)

        sums = each(n, gather, tuple(sums))

    for copy in exchanged:
        copy.wait()
    for k in range(slots):
        parts_of = [cuts_all[numbers[k] * SB // rows + i, k].astype(jnp.float32) for i in range(parts)]
        block = parts_of[0] if parts == 1 else jnp.concatenate(parts_of, axis=0)
        live = jnp.full((HALF, LANES), table[me, 0, slots]) > k
        keep = (times[k] >= 0) & (times[k] < samples) & live
        halves = []
        for h in range(2):
            rest = stencil(sums[2 * k + h]) - block[h * HALF : (h + 1) * HALF]
            halves.append(jnp.where(keep, rest, 0.0))
        whole = jnp.concatenate(halves, axis=0)
        windows[k] = pltpu.roll(whole, (LANES - starts[k]) & (LANES - 1), 1)

    for copy in sends:
        copy.wait()


def variation(n, place, image, halo):
    def units(volume, step_z):
        shape = volume.shape
        row = lax.broadcasted_iota(jnp.int32, shape, 0)
        below = jnp.concatenate([volume[1:], volume[shape[0] - 1 :]], axis=0)
        step_y = below - volume
        step_x = jnp.where(lane_iota(shape) < shape[1] - 1, ahead(volume, 1) - volume, 0.0)
        size = jnp.sqrt(step_z * step_z + step_y * step_y + step_x * step_x + TV_EPS)
        return step_z / size, step_y / size, step_x / size, row

    volume = image[0]
    before, after = halo[0], halo[1]
    is_first = jnp.full(volume.shape, place) == 0
    is_last = jnp.full(volume.shape, place) == n - 1
    lower_z, _, _, _ = units(before, volume - before)
    unit_z, unit_y, unit_x, row = units(volume, jnp.where(is_last, 0.0, after - volume))
    tv = jnp.where(is_first, 0.0, lower_z) - unit_z
    shifted_y = jnp.concatenate([jnp.zeros_like(unit_y[0:1]), unit_y[: unit_y.shape[0] - 1]], axis=0)
    tv = tv + shifted_y - unit_y
    tv = tv + jnp.where(lane_iota(volume.shape) >= 1, ahead(unit_x, -1), 0.0) - unit_x
    return tv


def update_kernel(
    n, ns, windows, wbuf, image, halo, turned, target, measured,
    out, residual, signals, grad, parts, send, recv
):
    mine = lax.axis_index("sen")
    place = lax.axis_index("vox")
    slots = wbuf.shape[0]
    rows, samples = measured.shape[1:]
    tiles = samples // LANES
    per = max(rows // SB, 1)
    barrier = pltpu.get_barrier_semaphore()
    for step in range(1, ns):
        pl.semaphore_signal(
            barrier, inc=1, device_id={"sen": (mine + step) % ns}, device_id_type=MESH
        )
    mask = block_mask(SB * WIN)
    left = lane_iota((SB, LANES)) < WIN
    part = None
    for k in range(slots):
        window = -stencil(windows[k])
        window = jnp.where(left, window, pltpu.roll(window, WIN, 1))
        spread = jnp.concatenate([window] * (SB * WIN // LANES), axis=1)
        spread = jnp.where(mask, spread, 0.0).astype(jnp.bfloat16)
        term = lax.dot_general(
            spread, wbuf[k], (((1,), (1,)), ((), ())), preferred_element_type=jnp.float32
        )
        part = term if part is None else part + term
    grad[...] = jnp.sum(part, axis=0, keepdims=True)
    pl.semaphore_wait(barrier, ns - 1)
    copies = []
    for step in range(1, ns):
        copy = pltpu.make_async_remote_copy(
            src_ref=grad, dst_ref=parts.at[mine], send_sem=send.at[step], recv_sem=recv.at[step],
            device_id={"sen": (mine + step) % ns}, device_id_type=MESH,
        )
        copy.start()
        copies.append(copy)

    home = place * rows // SB * tiles

    def fill(i, carry):
        wanted = home + i

        def add(j, sums):
            low, high = sums
            for k in range(slots):
                here = jnp.broadcast_to(target[j, k : k + 1], (HALF, LANES)) == wanted
                low = low + jnp.where(here, turned[j, k, 0:HALF], 0.0)
                high = high + jnp.where(here, turned[j, k, HALF:SB], 0.0)
            return low, high

        low, high = each(n, add, (jnp.zeros((HALF, LANES), jnp.float32),) * 2)
        line = i // tiles * SB
        column = pl.ds(pl.multiple_of(i % tiles * LANES, LANES), LANES)
        signals[pl.ds(pl.multiple_of(line, SB), HALF), column] = low
        signals[pl.ds(pl.multiple_of(line + HALF, HALF), HALF), column] = high
        return carry

    lax.fori_loop(0, per * tiles, fill, 0)

    for r in range(0, rows, HALF):
        line = r if rows >= SB else pl.multiple_of((place * rows + r) % SB // HALF * HALF, HALF)
        block = stencil_edges(signals[pl.ds(line, HALF)])
        if rows % HALF == 0:
            residual[0, r : r + HALF] = block - measured[0, r : r + HALF].astype(jnp.float32)
        else:
            which = jnp.full((rows, samples), (place * rows) % HALF)
            own = block[0:rows]
            for i in range(1, HALF // rows):
                own = jnp.where(which == i * rows, block[i * rows : (i + 1) * rows], own)
            residual[0] = own - measured[0].astype(jnp.float32)

    tv = variation(n, place, image, halo)
    for copy in copies:
        copy.wait()
    flat = None
    for index in range(ns):
        chosen = jnp.full(grad.shape, mine) == index
        term = jnp.where(chosen, grad[...], parts[index])
        flat = term if flat is None else flat + term
    volume = image[0]
    width = volume.shape[1]
    for r in range(volume.shape[0]):
        total = flat[:, r * width : (r + 1) * width]
        out[0, r : r + 1] = volume[r : r + 1] - STEP_SIZE * (total + TV_WEIGHT * tv[r : r + 1])


def store_kernel(image, residual, image_out, residual_out, sem):
    copies = []
    for i, (src, dst) in enumerate(((residual, residual_out), (image, image_out))):
        copy = pltpu.make_async_copy(src, dst, sem.at[i])
        copy.start()
        copies.append(copy)
    for copy in copies:
        copy.wait()


def on_device(image, weights, block_ids, offsets, counts, measured):
    n = lax.axis_size("vox")
    ns = lax.axis_size("sen")
    slots, voxels, cells = weights.shape[2:]
    rows, samples = measured.shape[1:]
    groups = (slots + 1) // 2
    chunks = 4
    vmem = pl.BlockSpec(memory_space=pltpu.VMEM)
    hbm = pl.BlockSpec(memory_space=pltpu.HBM)
    smem = pl.BlockSpec(memory_space=pltpu.SMEM)
    dma = pltpu.SemaphoreType.DMA
    shape = jax.ShapeDtypeStruct

    def pin(value):
        return pltpu.with_memory_space_constraint(value, pltpu.HBM)

    turned, target, windows, halo, held, image_held, measured_held = pl.pallas_call(
        functools.partial(gather_kernel, n, slots, chunks),
        out_shape=(
            shape((n, slots, SB, LANES), jnp.float32),
            shape((n, HALF, LANES), jnp.int32),
            shape((slots, SB, LANES), jnp.float32),
            shape((2,) + image.shape[1:], jnp.float32),
            shape((slots, voxels, cells), jnp.bfloat16),
            shape(image.shape, jnp.float32),
            shape(measured.shape, measured.dtype),
        ),
        in_specs=[hbm] * 4 + [smem, hbm],
        out_specs=(vmem,) * 7,
        scratch_shapes=[
            pltpu.VMEM(block_ids.shape, jnp.int32),
            pltpu.VMEM(offsets.shape, jnp.int32),
            pltpu.VMEM((groups, SB, LANES), jnp.float32),
            pltpu.VMEM((2, LANES), jnp.int32),
            pltpu.SMEM((n, 2, LANES), jnp.int32),
            pltpu.VMEM((n, groups, SB, LANES), jnp.float32),
            pltpu.VMEM((max(rows // SB, 1) * (samples // LANES), min(rows, SB), LANES), jnp.bfloat16),
            pltpu.VMEM((n, slots, min(rows, SB), LANES), jnp.bfloat16),
            pltpu.VMEM((n, slots, min(rows, SB), LANES), jnp.bfloat16),
            dma((slots, chunks)),
            dma((4,)),
            dma((2 + groups,)),
            dma((n,)),
            dma((n,)),
            dma((2,)),
            dma((2,)),
            dma((groups, n)),
            dma((groups, n)),
            dma((n,)),
            dma((n,)),
        ],
        compiler_params=pltpu.CompilerParams(
            collective_id=0, has_side_effects=True, vmem_limit_bytes=20 << 20
        ),
        name="gather_kernel",
    )(pin(image), pin(weights), pin(block_ids), pin(offsets), counts, pin(measured))

    image_next, residual = pl.pallas_call(
        functools.partial(update_kernel, n, ns),
        out_shape=(shape(image.shape, jnp.float32), shape(measured.shape, jnp.float32)),
        in_specs=[vmem] * 7,
        out_specs=(vmem, vmem),
        scratch_shapes=[
            pltpu.VMEM((max(rows, SB), samples), jnp.float32),
            pltpu.VMEM((1, voxels), jnp.float32),
            pltpu.VMEM((ns, 1, voxels), jnp.float32),
            dma((ns,)),
            dma((ns,)),
        ],
        compiler_params=pltpu.CompilerParams(
            collective_id=1, has_side_effects=True, vmem_limit_bytes=16 << 20
        ),
        name="update_kernel",
    )(windows, held, image_held, halo, turned, target, measured_held)

    return pl.pallas_call(
        store_kernel,
        out_shape=(shape(image.shape, jnp.float32), shape(measured.shape, jnp.float32)),
        in_specs=[vmem, vmem],
        out_specs=(hbm, hbm),
        scratch_shapes=[dma((2,))],
        compiler_params=pltpu.CompilerParams(vmem_limit_bytes=1 << 20),
        name="store_kernel",
    )(image_next, residual)


def solution(mesh):
    placed = (
        P("vox", None, None),
        P("vox", "sen", None, None, None),
        P("vox", "sen", None),
        P("vox", "sen", None),
        P("vox", "sen"),
        P("sen", "vox", None),
    )
    return jax.shard_map(
        on_device,
        mesh=mesh,
        in_specs=placed,
        out_specs=(P("vox", None, None), P("sen", "vox", None)),
        check_vma=False,
    )
```

```python
import functools

import jax
import jax.numpy as jnp
from jax import lax
from jax.experimental import pallas as pl
from jax.experimental.pallas import tpu as pltpu
from jax.sharding import PartitionSpec as P

SB = 16
WIN = 64
LANES = 128
HALF = 8
FAR = 1 << 16
UNROLL = 8

STEP_SIZE = 0.25
TV_WEIGHT = 0.3
TV_EPS = 0.01
C1 = 8.0 / 12.0
C2 = 1.0 / 12.0
MESH = pl.DeviceIdType.MESH


def lane_iota(shape):
    return lax.broadcasted_iota(jnp.int32, shape, len(shape) - 1)


def ahead(value, shift):
    length = value.shape[-1]
    return pltpu.roll(value, (-shift) % length, value.ndim - 1)


def stencil(value):
    return C2 * ahead(value, -2) - C1 * ahead(value, -1) + C1 * ahead(value, 1) - C2 * ahead(value, 2)


def stencil_edges(value):
    length = value.shape[-1]
    at = lane_iota(value.shape)
    total = jnp.where(at >= 2, C2 * ahead(value, -2), 0.0)
    total = total - jnp.where(at >= 1, C1 * ahead(value, -1), 0.0)
    total = total + jnp.where(at < length - 1, C1 * ahead(value, 1), 0.0)
    return total - jnp.where(at < length - 2, C2 * ahead(value, 2), 0.0)


def block_mask(width):
    row = lax.broadcasted_iota(jnp.int32, (SB, width), 0)
    return lane_iota((SB, width)) // WIN == row


def each(count, body, carry):
    if count > UNROLL:
        return lax.fori_loop(0, count, body, carry)
    for i in range(count):
        carry = body(i, carry)
    return carry


def variation(n, place, image, halo):
    def units(volume, step_z):
        shape = volume.shape
        row = lax.broadcasted_iota(jnp.int32, shape, 0)
        below = jnp.concatenate([volume[1:], volume[shape[0] - 1 :]], axis=0)
        step_y = below - volume
        step_x = jnp.where(lane_iota(shape) < shape[1] - 1, ahead(volume, 1) - volume, 0.0)
        size = jnp.sqrt(step_z * step_z + step_y * step_y + step_x * step_x + TV_EPS)
        return step_z / size, step_y / size, step_x / size, row

    volume = image[0]
    before, after = halo[0], halo[1]
    is_first = jnp.full(volume.shape, place) == 0
    is_last = jnp.full(volume.shape, place) == n - 1
    lower_z, _, _, _ = units(before, volume - before)
    unit_z, unit_y, unit_x, row = units(volume, jnp.where(is_last, 0.0, after - volume))
    tv = jnp.where(is_first, 0.0, lower_z) - unit_z
    shifted_y = jnp.concatenate([jnp.zeros_like(unit_y[0:1]), unit_y[: unit_y.shape[0] - 1]], axis=0)
    tv = tv + shifted_y - unit_y
    tv = tv + jnp.where(lane_iota(volume.shape) >= 1, ahead(unit_x, -1), 0.0) - unit_x
    return tv


def settle(ref, sem):
    pltpu.make_async_copy(ref, ref, sem).wait()


def step_kernel(
    n, ns, slots, chunks, image_in, weights, ids_in, offs_in, count, measured_in,
    out, residual,
    wbuf, turned_w, image, measured, tiled, ids, offs, meta, table, halo, mine, pieces_all,
    cuts, cuts_all, turned, target, signals, grad, parts,
    wsem, load_sem, meta_send, meta_recv, halo_send, halo_recv, piece_send, piece_recv,
    cut_send, cut_recv, grad_send, grad_recv,
):
    me = lax.axis_index("vox")
    layer = lax.axis_index("sen")
    voxels = weights.shape[3]
    depth = voxels // chunks
    rows, samples = measured.shape[1:]
    tiles = samples // LANES
    lines = min(rows, SB)
    strips = SB // lines
    per = max(rows // SB, 1)

    barrier = pltpu.get_barrier_semaphore()
    for step in range(1, n):
        pl.semaphore_signal(barrier, inc=1, device_id={"vox": (me + step) % n}, device_id_type=MESH)
    for step in range(1, ns):
        pl.semaphore_signal(barrier, inc=1, device_id={"sen": (layer + step) % ns}, device_id_type=MESH)

    arguments = []
    pairs = ((ids_in, ids), (offs_in, offs), (image_in, image), (measured_in, measured))
    for i, (src, dst) in enumerate(pairs):
        load = pltpu.make_async_copy(src, dst, load_sem.at[i])
        load.start()
        arguments.append(load)
    loads = []
    for k in range(slots):
        for q in range(chunks):
            part = pl.ds(q * depth, depth)
            load = pltpu.make_async_copy(weights.at[0, 0, k, part], wbuf.at[k, part], wsem.at[k, q])
            load.start(priority=1)
            loads.append(load)

    mask = block_mask(SB * WIN)
    alive = jnp.full((SB, LANES), count[0, 0])
    left = lane_iota((SB, LANES)) < WIN
    at = lane_iota((HALF, LANES))
    meta[...] = jnp.zeros_like(meta)
    arguments[0].wait()
    arguments[1].wait()
    meta[0:1, 0:slots] = ids[0]
    meta[1:2, 0:slots] = offs[0]
    pl.semaphore_wait(barrier, n - 1 + ns - 1)

    def remote(src, dst, send, recv, axis, to):
        pltpu.make_async_remote_copy(
            src_ref=src, dst_ref=dst, send_sem=send, recv_sem=recv,
            device_id={axis: to}, device_id_type=MESH,
        ).start()

    for step in range(1, n):
        remote(meta, table.at[me], meta_send, meta_recv, "vox", (me + step) % n)
    pltpu.make_async_copy(meta, table.at[me], meta_recv).start()
    arguments[2].wait()
    for side, to in ((0, (me + 1) % n), (1, (me + n - 1) % n)):
        remote(image.at[0], halo.at[side], halo_send, halo_recv.at[side], "vox", to)
    low = image[0].astype(jnp.bfloat16)
    flat = jnp.concatenate([low[r : r + 1] for r in range(low.shape[0])], axis=1)
    flat = jnp.broadcast_to(flat, (SB, voxels))
    arguments[3].wait()
    for i in range(per * tiles):
        tiled[i] = measured[0, i // tiles * SB : i // tiles * SB + lines, i % tiles * LANES : (i % tiles + 1) * LANES]

    def forward(k):
        total = jnp.zeros((SB, SB * WIN), jnp.float32)
        for q in range(chunks):
            loads[k * chunks + q].wait()
            total = total + jnp.dot(
                flat[:, q * depth : (q + 1) * depth],
                wbuf[k, q * depth : (q + 1) * depth],
                preferred_element_type=jnp.float32,
            )
        total = jnp.where(mask, total, 0.0)
        tile = total[:, 0:LANES]
        for g in range(1, SB * WIN // LANES):
            tile = tile + total[:, g * LANES : (g + 1) * LANES]
        tile = tile + pltpu.roll(tile, WIN, 1)
        return jnp.where(alive > k, tile, 0.0)

    packed = None
    for k in range(slots):
        tile = forward(k)
        packed = jnp.where(left, tile, 0.0) if k % 2 == 0 else jnp.where(left, packed, tile)
        if k % 2 == 1 or k == slots - 1:
            g = k // 2
            mine[g] = packed
            for step in range(1, n):
                remote(mine.at[g], pieces_all.at[g, me], piece_send, piece_recv.at[g], "vox", (me + step) % n)
            pltpu.make_async_copy(mine.at[g], pieces_all.at[g, me], piece_recv.at[g]).start()

    settle(table, meta_recv)

    def cut(j):
        across = lane_iota((lines, LANES))
        for k in range(slots):
            near = jnp.clip(table[j, 0, k] - me * per, 0, per - 1) * tiles
            base = jnp.maximum(table[j, 1, k] - 2, 0)
            first = base // LANES
            after = jnp.minimum(first + 1, tiles - 1)
            one = tiled[near + first].astype(jnp.float32)
            two = tiled[near + after].astype(jnp.float32)
            cuts[j, k] = jnp.where(across >= base % LANES, one, two).astype(cuts.dtype)

    for step in range(n - 1, 0, -1):
        to = (me + step) % n
        cut(to)
        remote(cuts.at[to], cuts_all.at[me], cut_send, cut_recv, "vox", to)
    cut(me)
    pltpu.make_async_copy(cuts.at[me], cuts_all.at[me], cut_recv).start()

    for k in range(slots):
        turned_w[k] = wbuf[k].T

    numbers = [table[me, 0, k] for k in range(slots)]
    starts = [table[me, 1, k] for k in range(slots)]
    times = [start - WIN // 2 + ((at - start + WIN // 2) & (LANES - 1)) for start in starts]
    keys = [number * FAR + time for number, time in zip(numbers, times)]
    lane = lane_iota((1, LANES))

    sums = (jnp.zeros((HALF, LANES), jnp.float32),) * (slots * 2)
    for g in range(pieces_all.shape[0]):
        settle(pieces_all.at[g], piece_recv.at[g])

        def gather(j, sums, g=g):
            sums = list(sums)
            packed = pieces_all[g, j]
            for k in range(2 * g, min(2 * g + 2, slots)):
                number, start = table[j, 0, k], table[j, 1, k]
                piece = pltpu.roll(packed, (start + (k % 2) * WIN) & (LANES - 1), 1)
                turned[j, k] = piece
                since = (lane - start) & (LANES - 1)
                spot = number * tiles + lax.shift_right_logical(since + start, 7)
                target[j, k : k + 1] = jnp.where(since < WIN, spot, -1)
                key = number * FAR + start
                for i in range(slots):
                    since = keys[i] - key
                    inside = (since >= 0) & (since < WIN)
                    for h in range(2):
                        part = piece[h * HALF : (h + 1) * HALF]
                        sums[2 * i + h] = sums[2 * i + h] + jnp.where(inside, part, 0.0)
            return tuple(sums)

        sums = each(n, gather, sums)

    derived = [stencil(value) for value in sums]
    settle(cuts_all, cut_recv)
    spreads = []
    for k in range(slots):
        stripes = [cuts_all[numbers[k] * SB // rows + i, k].astype(jnp.float32) for i in range(strips)]
        block = stripes[0] if strips == 1 else jnp.concatenate(stripes, axis=0)
        keep = (times[k] >= 0) & (times[k] < samples) & (jnp.full((HALF, LANES), count[0, 0]) > k)
        halves = []
        for h in range(2):
            rest = jnp.where(keep, derived[2 * k + h] - block[h * HALF : (h + 1) * HALF], 0.0)
            halves.append(-stencil(rest))
        window = jnp.concatenate(halves, axis=0)
        even = pltpu.roll(window, (LANES - starts[k]) & (LANES - 1), 1)
        odd = pltpu.roll(window, (LANES + WIN - starts[k]) & (LANES - 1), 1)
        window = jnp.where(left, even, odd)
        spread = jnp.concatenate([window] * (SB * WIN // LANES), axis=1)
        spreads.append(jnp.where(mask, spread, 0.0).astype(jnp.bfloat16))
    part = None
    for k in range(slots):
        term = jnp.dot(spreads[k], turned_w[k], preferred_element_type=jnp.float32)
        part = term if part is None else part + term
    grad[...] = jnp.sum(part, axis=0, keepdims=True)
    for step in range(ns - 1, 0, -1):
        remote(grad, parts.at[layer], grad_send, grad_recv, "sen", (layer + step) % ns)
    pltpu.make_async_copy(grad, parts.at[layer], grad_recv).start()

    home = me * rows // SB * tiles

    def fill(i, carry):
        wanted = home + i

        def add(j, sums):
            low, high = sums
            for k in range(slots):
                here = jnp.broadcast_to(target[j, k : k + 1], (HALF, LANES)) == wanted
                low = low + jnp.where(here, turned[j, k, 0:HALF], 0.0)
                high = high + jnp.where(here, turned[j, k, HALF:SB], 0.0)
            return low, high

        low, high = each(n, add, (jnp.zeros((HALF, LANES), jnp.float32),) * 2)
        line = i // tiles * SB
        column = pl.ds(pl.multiple_of(i % tiles * LANES, LANES), LANES)
        signals[pl.ds(pl.multiple_of(line, SB), HALF), column] = low
        signals[pl.ds(pl.multiple_of(line + HALF, HALF), HALF), column] = high
        return carry

    lax.fori_loop(0, per * tiles, fill, 0)

    for r in range(0, rows, HALF):
        line = r if rows >= SB else pl.multiple_of((me * rows + r) % SB // HALF * HALF, HALF)
        block = stencil_edges(signals[pl.ds(line, HALF)])
        if rows % HALF == 0:
            residual[0, r : r + HALF] = block - measured[0, r : r + HALF].astype(jnp.float32)
        else:
            which = jnp.full((rows, samples), (me * rows) % HALF)
            own = block[0:rows]
            for i in range(1, HALF // rows):
                own = jnp.where(which == i * rows, block[i * rows : (i + 1) * rows], own)
            residual[0] = own - measured[0].astype(jnp.float32)

    settle(halo.at[0], halo_recv.at[0])
    settle(halo.at[1], halo_recv.at[1])
    tv = variation(n, me, image, halo)
    settle(table.at[pl.ds(0, n - 1)], meta_send)
    settle(halo, halo_send)
    settle(pieces_all.at[:, pl.ds(0, n - 1)], piece_send)
    settle(cuts_all.at[pl.ds(0, n - 1)], cut_send)
    settle(parts, grad_recv)
    flat = parts[0]
    for index in range(1, ns):
        flat = flat + parts[index]
    volume = image[0]
    width = volume.shape[1]
    for r in range(volume.shape[0]):
        total = flat[:, r * width : (r + 1) * width]
        out[0, r : r + 1] = volume[r : r + 1] - STEP_SIZE * (total + TV_WEIGHT * tv[r : r + 1])
    settle(parts.at[pl.ds(0, ns - 1)], grad_send)


def store_kernel(image, residual, image_out, residual_out, sem):
    copies = []
    for i, (src, dst) in enumerate(((residual, residual_out), (image, image_out))):
        copy = pltpu.make_async_copy(src, dst, sem.at[i])
        copy.start()
        copies.append(copy)
    for copy in copies:
        copy.wait()


def on_device(image, weights, block_ids, offsets, counts, measured):
    n = lax.axis_size("vox")
    ns = lax.axis_size("sen")
    slots, voxels, cells = weights.shape[2:]
    rows, samples = measured.shape[1:]
    groups = (slots + 1) // 2
    lines = min(rows, SB)
    chunks = 4
    vmem = pl.BlockSpec(memory_space=pltpu.VMEM)
    hbm = pl.BlockSpec(memory_space=pltpu.HBM)
    smem = pl.BlockSpec(memory_space=pltpu.SMEM)
    dma = pltpu.SemaphoreType.DMA
    shape = jax.ShapeDtypeStruct

    def pin(value):
        return pltpu.with_memory_space_constraint(value, pltpu.HBM)

    image_next, residual = pl.pallas_call(
        functools.partial(step_kernel, n, ns, slots, chunks),
        out_shape=(shape(image.shape, jnp.float32), shape(measured.shape, jnp.float32)),
        in_specs=[hbm] * 4 + [smem, hbm],
        out_specs=(vmem, vmem),
        scratch_shapes=[
            pltpu.VMEM((slots, voxels, cells), jnp.bfloat16),
            pltpu.VMEM((slots, cells, voxels), jnp.bfloat16),
            pltpu.VMEM(image.shape, jnp.float32),
            pltpu.VMEM(measured.shape, measured.dtype),
            pltpu.VMEM((max(rows // SB, 1) * (samples // LANES), lines, LANES), jnp.bfloat16),
            pltpu.VMEM(block_ids.shape, jnp.int32),
            pltpu.VMEM(offsets.shape, jnp.int32),
            pltpu.VMEM((2, LANES), jnp.int32),
            pltpu.SMEM((n, 2, LANES), jnp.int32),
            pltpu.VMEM((2,) + image.shape[1:], jnp.float32),
            pltpu.VMEM((groups, SB, LANES), jnp.float32),
            pltpu.VMEM((groups, n, SB, LANES), jnp.float32),
            pltpu.VMEM((n, slots, lines, LANES), jnp.bfloat16),
            pltpu.VMEM((n, slots, lines, LANES), jnp.bfloat16),
            pltpu.VMEM((n, slots, SB, LANES), jnp.float32),
            pltpu.VMEM((n, HALF, LANES), jnp.int32),
            pltpu.VMEM((max(rows, SB), samples), jnp.float32),
            pltpu.VMEM((1, voxels), jnp.float32),
            pltpu.VMEM((ns, 1, voxels), jnp.float32),
            dma((slots, chunks)),
            dma((4,)),
            dma,
            dma,
            dma,
            dma((2,)),
            dma,
            dma((groups,)),
            dma,
            dma,
            dma,
            dma,
        ],
        compiler_params=pltpu.CompilerParams(
            collective_id=0, has_side_effects=True, vmem_limit_bytes=40 << 20
        ),
        name="step_kernel",
    )(pin(image), pin(weights), pin(block_ids), pin(offsets), counts, pin(measured))

    return pl.pallas_call(
        store_kernel,
        out_shape=(shape(image.shape, jnp.float32), shape(measured.shape, jnp.float32)),
        in_specs=[vmem, vmem],
        out_specs=(hbm, hbm),
        scratch_shapes=[dma((2,))],
        compiler_params=pltpu.CompilerParams(vmem_limit_bytes=1 << 20),
        name="store_kernel",
    )(image_next, residual)


def solution(mesh):
    placed = (
        P("vox", None, None),
        P("vox", "sen", None, None, None),
        P("vox", "sen", None),
        P("vox", "sen", None),
        P("vox", "sen"),
        P("sen", "vox", None),
    )
    return jax.shard_map(
        on_device,
        mesh=mesh,
        in_specs=placed,
        out_specs=(P("vox", None, None), P("sen", "vox", None)),
        check_vma=False,
    )
```

```python
import functools

import jax
import jax.numpy as jnp
from jax import lax
from jax.experimental import pallas as pl
from jax.experimental.pallas import tpu as pltpu
from jax.sharding import PartitionSpec as P

SB = 16
WIN = 64
LANES = 128
HALF = 8
EDGE = 2
SPAN = WIN + 2 * EDGE
FAR = 1 << 16
UNROLL = 8

STEP_SIZE = 0.25
TV_WEIGHT = 0.3
TV_EPS = 0.01
C1 = 8.0 / 12.0
C2 = 1.0 / 12.0
MESH = pl.DeviceIdType.MESH


def lane_iota(shape):
    return lax.broadcasted_iota(jnp.int32, shape, len(shape) - 1)


def ahead(value, shift):
    length = value.shape[-1]
    return pltpu.roll(value, (-shift) % length, value.ndim - 1)


def stencil(value):
    return C2 * ahead(value, -2) - C1 * ahead(value, -1) + C1 * ahead(value, 1) - C2 * ahead(value, 2)


def stencil_edges(value):
    length = value.shape[-1]
    at = lane_iota(value.shape)
    total = jnp.where(at >= 2, C2 * ahead(value, -2), 0.0)
    total = total - jnp.where(at >= 1, C1 * ahead(value, -1), 0.0)
    total = total + jnp.where(at < length - 1, C1 * ahead(value, 1), 0.0)
    return total - jnp.where(at < length - 2, C2 * ahead(value, 2), 0.0)


def block_mask(width):
    row = lax.broadcasted_iota(jnp.int32, (SB, width), 0)
    return lane_iota((SB, width)) // WIN == row


def peer(me, count, step):
    return me ^ step if count & (count - 1) == 0 else (me + step) % count


def each(count, body, carry):
    if count > UNROLL:
        return lax.fori_loop(0, count, body, carry)
    for i in range(count):
        carry = body(i, carry)
    return carry


def variation(n, place, image, halo):
    def units(volume, step_z):
        shape = volume.shape
        row = lax.broadcasted_iota(jnp.int32, shape, 0)
        below = jnp.concatenate([volume[1:], volume[shape[0] - 1 :]], axis=0)
        step_y = below - volume
        step_x = jnp.where(lane_iota(shape) < shape[1] - 1, ahead(volume, 1) - volume, 0.0)
        size = jnp.sqrt(step_z * step_z + step_y * step_y + step_x * step_x + TV_EPS)
        return step_z / size, step_y / size, step_x / size, row

    volume = image[0]
    before, after = halo[0], halo[1]
    is_first = jnp.full(volume.shape, place) == 0
    is_last = jnp.full(volume.shape, place) == n - 1
    lower_z, _, _, _ = units(before, volume - before)
    unit_z, unit_y, unit_x, row = units(volume, jnp.where(is_last, 0.0, after - volume))
    tv = jnp.where(is_first, 0.0, lower_z) - unit_z
    shifted_y = jnp.concatenate([jnp.zeros_like(unit_y[0:1]), unit_y[: unit_y.shape[0] - 1]], axis=0)
    tv = tv + shifted_y - unit_y
    tv = tv + jnp.where(lane_iota(volume.shape) >= 1, ahead(unit_x, -1), 0.0) - unit_x
    return tv


def settle(ref, sem):
    pltpu.make_async_copy(ref, ref, sem).wait()


def step_kernel(
    n, ns, slots, chunks, image_in, weights, ids_in, offs_in, count, measured_in,
    out, residual,
    wbuf, turned_w, image, measured, tiled, ids, offs, meta, table, halo, mine, pieces_all, lone, lone_all,
    cuts, cuts_all, turned, target, signals, grad, parts,
    wsem, load_sem, meta_send, meta_recv, halo_send, halo_recv, piece_send, piece_recv, lone_recv,
    cut_send, cut_recv, grad_send, grad_recv,
):
    me = lax.axis_index("vox")
    layer = lax.axis_index("sen")
    voxels = weights.shape[3]
    depth = voxels // chunks
    rows, samples = measured.shape[1:]
    tiles = samples // LANES
    lines = min(rows, SB)
    strips = SB // lines
    per = max(rows // SB, 1)

    barrier = pltpu.get_barrier_semaphore()
    for step in range(1, n):
        pl.semaphore_signal(barrier, inc=1, device_id={"vox": (me + step) % n}, device_id_type=MESH)
    for step in range(1, ns):
        pl.semaphore_signal(barrier, inc=1, device_id={"sen": (layer + step) % ns}, device_id_type=MESH)

    arguments = []
    pairs = ((ids_in, ids), (offs_in, offs), (image_in, image), (measured_in, measured))
    for i, (src, dst) in enumerate(pairs):
        load = pltpu.make_async_copy(src, dst, load_sem.at[i])
        load.start()
        arguments.append(load)
    loads = []
    for k in range(slots):
        for q in range(chunks):
            part = pl.ds(q * depth, depth)
            load = pltpu.make_async_copy(weights.at[0, 0, k, part], wbuf.at[k, part], wsem.at[k, q])
            load.start(priority=1)
            loads.append(load)

    mask = block_mask(SB * WIN)
    alive = jnp.full((SB, LANES), count[0, 0])
    left = lane_iota((SB, LANES)) < WIN
    at = lane_iota((HALF, LANES))
    meta[...] = jnp.zeros_like(meta)
    arguments[0].wait()
    arguments[1].wait()
    meta[0:1, 0:slots] = ids[0]
    meta[1:2, 0:slots] = offs[0]
    pl.semaphore_wait(barrier, n - 1 + ns - 1)

    def remote(src, dst, send, recv, axis, to):
        pltpu.make_async_remote_copy(
            src_ref=src, dst_ref=dst, send_sem=send, recv_sem=recv,
            device_id={axis: to}, device_id_type=MESH,
        ).start()

    for step in range(1, n):
        remote(meta, table.at[me], meta_send, meta_recv, "vox", peer(me, n, n - step))
    pltpu.make_async_copy(meta, table.at[me], meta_recv).start()
    arguments[2].wait()
    for side, to in ((0, (me + 1) % n), (1, (me + n - 1) % n)):
        remote(image.at[0], halo.at[side], halo_send, halo_recv.at[side], "vox", to)
    low = image[0].astype(jnp.bfloat16)
    flat = jnp.concatenate([low[r : r + 1] for r in range(low.shape[0])], axis=1)
    flat = jnp.broadcast_to(flat, (SB, voxels))
    arguments[3].wait()
    for i in range(per * tiles):
        tiled[i] = measured[0, i // tiles * SB : i // tiles * SB + lines, i % tiles * LANES : (i % tiles + 1) * LANES]

    def forward(k):
        total = jnp.zeros((SB, SB * WIN), jnp.float32)
        for q in range(chunks):
            loads[k * chunks + q].wait()
            total = total + jnp.dot(
                flat[:, q * depth : (q + 1) * depth],
                wbuf[k, q * depth : (q + 1) * depth],
                preferred_element_type=jnp.float32,
            )
        total = jnp.where(mask, total, 0.0)
        tile = total[:, 0:LANES]
        for g in range(1, SB * WIN // LANES):
            tile = tile + total[:, g * LANES : (g + 1) * LANES]
        tile = tile + pltpu.roll(tile, WIN, 1)
        return jnp.where(alive > k, tile, 0.0)

    def spread_out(src, dst, recv):
        for step in range(1, n):
            remote(src, dst, piece_send, recv, "vox", peer(me, n, n - step))
        pltpu.make_async_copy(src, dst, recv).start()

    first = None
    for k in range(slots):
        tile = forward(k)
        if k % 2 == 1:
            mine[k // 2] = jnp.where(left, first, tile)
            spread_out(mine.at[k // 2], pieces_all.at[k // 2, me], piece_recv.at[k // 2])
        elif k == slots - 1:
            lone[...] = jnp.where(left[0:HALF], tile[0:HALF], tile[HALF:SB])
            spread_out(lone, lone_all.at[me], lone_recv)
        first = tile

    settle(table, meta_recv)

    def cut(j):
        across = lane_iota((lines, LANES))
        spans = []
        for k in range(slots):
            near = jnp.clip(table[j, 0, k] - me * per, 0, per - 1) * tiles
            start = table[j, 1, k]
            base = jnp.maximum(start - EDGE, 0)
            first = base // LANES
            after = jnp.minimum(first + 1, tiles - 1)
            one = tiled[near + first].astype(jnp.float32)
            two = tiled[near + after].astype(jnp.float32)
            span = jnp.where(across >= base % LANES, one, two)
            spans.append(pltpu.roll(span, (k * SPAN + EDGE - start) & (LANES - 1), 1))
        for i in range(cuts.shape[1]):
            packed = None
            for k in range(slots):
                begin = k * SPAN - i * LANES
                if begin + SPAN <= 0 or begin >= LANES:
                    continue
                packed = spans[k] if packed is None else jnp.where(across >= begin, spans[k], packed)
            cuts[j, i] = packed.astype(cuts.dtype)

    order = [peer(me, n, step) for step in range(n - 1, 0, -1)]
    for some in (order[:2], order[2:]):
        for to in some:
            cut(to)
        for to in some:
            remote(cuts.at[to], cuts_all.at[me], cut_send, cut_recv, "vox", to)
    cut(me)
    pltpu.make_async_copy(cuts.at[me], cuts_all.at[me], cut_recv).start()

    for k in range(slots):
        turned_w[k] = wbuf[k].T

    numbers = [table[me, 0, k] for k in range(slots)]
    starts = [table[me, 1, k] for k in range(slots)]
    times = [start - WIN // 2 + ((at - start + WIN // 2) & (LANES - 1)) for start in starts]
    keys = [number * FAR + time for number, time in zip(numbers, times)]
    lane = lane_iota((1, LANES))

    sums = (jnp.zeros((HALF, LANES), jnp.float32),) * (slots * 2)
    def gather(j, sums, ks, load):
        sums = list(sums)
        for k in ks:
            number, start = table[j, 0, k], table[j, 1, k]
            piece = load(j, k, start)
            turned[j, k] = piece
            since = (lane - start) & (LANES - 1)
            spot = number * tiles + lax.shift_right_logical(since + start, 7)
            target[j, k : k + 1] = jnp.where(since < WIN, spot, -1)
            key = number * FAR + start
            for i in range(slots):
                since = keys[i] - key
                inside = (since >= 0) & (since < WIN)
                for h in range(2):
                    part = piece[h * HALF : (h + 1) * HALF]
                    sums[2 * i + h] = sums[2 * i + h] + jnp.where(inside, part, 0.0)
        return tuple(sums)

    def load_pair(j, k, start):
        return pltpu.roll(pieces_all[k // 2, j], (start + (k % 2) * WIN) & (LANES - 1), 1)

    def load_lone(j, k, start):
        upper = pltpu.roll(lone_all[j], start & (LANES - 1), 1)
        lower = pltpu.roll(lone_all[j], (start + WIN) & (LANES - 1), 1)
        return jnp.concatenate([upper, lower], axis=0)

    for g in range(slots // 2):
        settle(pieces_all.at[g], piece_recv.at[g])
        sums = each(n, functools.partial(gather, ks=(2 * g, 2 * g + 1), load=load_pair), sums)
    if slots % 2:
        settle(lone_all, lone_recv)
        sums = each(n, functools.partial(gather, ks=(slots - 1,), load=load_lone), sums)

    derived = []
    for k in range(slots):
        value = jnp.concatenate([stencil(sums[2 * k]), stencil(sums[2 * k + 1])], axis=0)
        derived.append(pltpu.roll(value, (LANES + EDGE - starts[k]) & (LANES - 1), 1))
    wide = lane_iota((SB, LANES))
    settle(cuts_all, cut_recv)
    spreads = []
    for k in range(slots):
        stripes = []
        for i in range(strips):
            owner = numbers[k] * SB // rows + i
            begin, last = k * SPAN, (k + 1) * SPAN - 1
            stripe = cuts_all[owner, begin // LANES].astype(jnp.float32)
            if last // LANES > begin // LANES:
                follow = cuts_all[owner, last // LANES].astype(jnp.float32)
                stripe = jnp.where(lane_iota((lines, LANES)) >= begin % LANES, stripe, follow)
            stripes.append(stripe)
        block = stripes[0] if strips == 1 else jnp.concatenate(stripes, axis=0)
        if k:
            block = pltpu.roll(block, (-k * SPAN) % LANES, 1)
        time = wide + (starts[k] - EDGE)
        keep = (time >= 0) & (time < samples) & (jnp.full((SB, LANES), count[0, 0]) > k)
        window = -stencil(jnp.where(keep, derived[k] - block, 0.0))
        window = jnp.where(left, ahead(window, EDGE), ahead(window, EDGE - WIN))
        spread = jnp.concatenate([window] * (SB * WIN // LANES), axis=1)
        spreads.append(jnp.where(mask, spread, 0.0).astype(jnp.bfloat16))
    part = None
    for k in range(slots):
        term = jnp.dot(spreads[k], turned_w[k], preferred_element_type=jnp.float32)
        part = term if part is None else part + term
    grad[...] = jnp.sum(part, axis=0, keepdims=True)
    for step in range(ns - 1, 0, -1):
        remote(grad, parts.at[layer], grad_send, grad_recv, "sen", (layer + step) % ns)
    pltpu.make_async_copy(grad, parts.at[layer], grad_recv).start()

    home = me * rows // SB * tiles

    def fill(i, carry):
        wanted = home + i

        def add(j, sums):
            low, high = sums
            for k in range(slots):
                here = jnp.broadcast_to(target[j, k : k + 1], (HALF, LANES)) == wanted
                low = low + jnp.where(here, turned[j, k, 0:HALF], 0.0)
                high = high + jnp.where(here, turned[j, k, HALF:SB], 0.0)
            return low, high

        low, high = each(n, add, (jnp.zeros((HALF, LANES), jnp.float32),) * 2)
        line = i // tiles * SB
        column = pl.ds(pl.multiple_of(i % tiles * LANES, LANES), LANES)
        signals[pl.ds(pl.multiple_of(line, SB), HALF), column] = low
        signals[pl.ds(pl.multiple_of(line + HALF, HALF), HALF), column] = high
        return carry

    lax.fori_loop(0, per * tiles, fill, 0)

    for r in range(0, rows, HALF):
        line = r if rows >= SB else pl.multiple_of((me * rows + r) % SB // HALF * HALF, HALF)
        block = stencil_edges(signals[pl.ds(line, HALF)])
        if rows % HALF == 0:
            residual[0, r : r + HALF] = block - measured[0, r : r + HALF].astype(jnp.float32)
        else:
            which = jnp.full((rows, samples), (me * rows) % HALF)
            own = block[0:rows]
            for i in range(1, HALF // rows):
                own = jnp.where(which == i * rows, block[i * rows : (i + 1) * rows], own)
            residual[0] = own - measured[0].astype(jnp.float32)

    settle(halo.at[0], halo_recv.at[0])
    settle(halo.at[1], halo_recv.at[1])
    tv = variation(n, me, image, halo)
    settle(table.at[pl.ds(0, n - 1)], meta_send)
    settle(halo, halo_send)
    settle(pieces_all.at[:, pl.ds(0, n - 1)], piece_send)
    if slots % 2:
        settle(lone_all.at[pl.ds(0, n - 1)], piece_send)
    settle(cuts_all.at[pl.ds(0, n - 1)], cut_send)
    settle(parts, grad_recv)
    flat = parts[0]
    for index in range(1, ns):
        flat = flat + parts[index]
    volume = image[0]
    width = volume.shape[1]
    for r in range(volume.shape[0]):
        total = flat[:, r * width : (r + 1) * width]
        out[0, r : r + 1] = volume[r : r + 1] - STEP_SIZE * (total + TV_WEIGHT * tv[r : r + 1])
    settle(parts.at[pl.ds(0, ns - 1)], grad_send)


def store_kernel(image, residual, image_out, residual_out, sem):
    copies = []
    for i, (src, dst) in enumerate(((residual, residual_out), (image, image_out))):
        copy = pltpu.make_async_copy(src, dst, sem.at[i])
        copy.start()
        copies.append(copy)
    for copy in copies:
        copy.wait()


def on_device(image, weights, block_ids, offsets, counts, measured):
    n = lax.axis_size("vox")
    ns = lax.axis_size("sen")
    slots, voxels, cells = weights.shape[2:]
    rows, samples = measured.shape[1:]
    pairs = slots // 2
    lines = min(rows, SB)
    chunks = 2
    vmem = pl.BlockSpec(memory_space=pltpu.VMEM)
    hbm = pl.BlockSpec(memory_space=pltpu.HBM)
    smem = pl.BlockSpec(memory_space=pltpu.SMEM)
    dma = pltpu.SemaphoreType.DMA
    shape = jax.ShapeDtypeStruct

    def pin(value):
        return pltpu.with_memory_space_constraint(value, pltpu.HBM)

    image_next, residual = pl.pallas_call(
        functools.partial(step_kernel, n, ns, slots, chunks),
        out_shape=(shape(image.shape, jnp.float32), shape(measured.shape, jnp.float32)),
        in_specs=[hbm] * 4 + [smem, hbm],
        out_specs=(vmem, vmem),
        scratch_shapes=[
            pltpu.VMEM((slots, voxels, cells), jnp.bfloat16),
            pltpu.VMEM((slots, cells, voxels), jnp.bfloat16),
            pltpu.VMEM(image.shape, jnp.float32),
            pltpu.VMEM(measured.shape, measured.dtype),
            pltpu.VMEM((max(rows // SB, 1) * (samples // LANES), lines, LANES), jnp.bfloat16),
            pltpu.VMEM(block_ids.shape, jnp.int32),
            pltpu.VMEM(offsets.shape, jnp.int32),
            pltpu.VMEM((2, LANES), jnp.int32),
            pltpu.SMEM((n, 2, LANES), jnp.int32),
            pltpu.VMEM((2,) + image.shape[1:], jnp.float32),
            pltpu.VMEM((pairs, SB, LANES), jnp.float32),
            pltpu.VMEM((pairs, n, SB, LANES), jnp.float32),
            pltpu.VMEM((HALF, LANES), jnp.float32),
            pltpu.VMEM((n, HALF, LANES), jnp.float32),
            pltpu.VMEM((n, pl.cdiv(slots * SPAN, LANES), lines, LANES), jnp.bfloat16),
            pltpu.VMEM((n, pl.cdiv(slots * SPAN, LANES), lines, LANES), jnp.bfloat16),
            pltpu.VMEM((n, slots, SB, LANES), jnp.float32),
            pltpu.VMEM((n, HALF, LANES), jnp.int32),
            pltpu.VMEM((max(rows, SB), samples), jnp.float32),
            pltpu.VMEM((1, voxels), jnp.float32),
            pltpu.VMEM((ns, 1, voxels), jnp.float32),
            dma((slots, chunks)),
            dma((4,)),
            dma,
            dma,
            dma,
            dma((2,)),
            dma,
            dma((pairs,)),
            dma,
            dma,
            dma,
            dma,
            dma,
        ],
        compiler_params=pltpu.CompilerParams(
            collective_id=0, has_side_effects=True, vmem_limit_bytes=40 << 20
        ),
        name="step_kernel",
    )(pin(image), pin(weights), pin(block_ids), pin(offsets), counts, pin(measured))

    return pl.pallas_call(
        store_kernel,
        out_shape=(shape(image.shape, jnp.float32), shape(measured.shape, jnp.float32)),
        in_specs=[vmem, vmem],
        out_specs=(hbm, hbm),
        scratch_shapes=[dma((2,))],
        compiler_params=pltpu.CompilerParams(vmem_limit_bytes=1 << 20),
        name="store_kernel",
    )(image_next, residual)


def solution(mesh):
    placed = (
        P("vox", None, None),
        P("vox", "sen", None, None, None),
        P("vox", "sen", None),
        P("vox", "sen", None),
        P("vox", "sen"),
        P("sen", "vox", None),
    )
    return jax.shard_map(
        on_device,
        mesh=mesh,
        in_specs=placed,
        out_specs=(P("vox", None, None), P("sen", "vox", None)),
        check_vma=False,
    )
```

```python
import functools

import jax
import jax.numpy as jnp
from jax import lax
from jax.experimental import pallas as pl
from jax.experimental.pallas import tpu as pltpu
from jax.sharding import PartitionSpec as P

SB = 16
WIN = 64
LANES = 128
HALF = 8
EDGE = 2
SPAN = WIN + 2 * EDGE
FAR = 1 << 16
UNROLL = 8
STORES = 4

STEP_SIZE = 0.25
TV_WEIGHT = 0.3
TV_EPS = 0.01
C1 = 8.0 / 12.0
C2 = 1.0 / 12.0
MESH = pl.DeviceIdType.MESH


def lane_iota(shape):
    return lax.broadcasted_iota(jnp.int32, shape, len(shape) - 1)


def ahead(value, shift):
    length = value.shape[-1]
    return pltpu.roll(value, (-shift) % length, value.ndim - 1)


def stencil(value):
    return C2 * ahead(value, -2) - C1 * ahead(value, -1) + C1 * ahead(value, 1) - C2 * ahead(value, 2)


def stencil_edges(value):
    length = value.shape[-1]
    at = lane_iota(value.shape)
    total = jnp.where(at >= 2, C2 * ahead(value, -2), 0.0)
    total = total - jnp.where(at >= 1, C1 * ahead(value, -1), 0.0)
    total = total + jnp.where(at < length - 1, C1 * ahead(value, 1), 0.0)
    return total - jnp.where(at < length - 2, C2 * ahead(value, 2), 0.0)


def block_mask(width):
    row = lax.broadcasted_iota(jnp.int32, (SB, width), 0)
    return lane_iota((SB, width)) // WIN == row


def peer(me, count, step):
    return me ^ step if count & (count - 1) == 0 else (me + step) % count


def each(count, body, carry):
    if count > UNROLL:
        return lax.fori_loop(0, count, body, carry)
    for i in range(count):
        carry = body(i, carry)
    return carry


def variation(n, place, image, halo):
    def units(volume, step_z):
        shape = volume.shape
        row = lax.broadcasted_iota(jnp.int32, shape, 0)
        below = jnp.concatenate([volume[1:], volume[shape[0] - 1 :]], axis=0)
        step_y = below - volume
        step_x = jnp.where(lane_iota(shape) < shape[1] - 1, ahead(volume, 1) - volume, 0.0)
        size = jnp.sqrt(step_z * step_z + step_y * step_y + step_x * step_x + TV_EPS)
        return step_z / size, step_y / size, step_x / size, row

    volume = image[0]
    before, after = halo[0], halo[1]
    is_first = jnp.full(volume.shape, place) == 0
    is_last = jnp.full(volume.shape, place) == n - 1
    lower_z, _, _, _ = units(before, volume - before)
    unit_z, unit_y, unit_x, row = units(volume, jnp.where(is_last, 0.0, after - volume))
    tv = jnp.where(is_first, 0.0, lower_z) - unit_z
    shifted_y = jnp.concatenate([jnp.zeros_like(unit_y[0:1]), unit_y[: unit_y.shape[0] - 1]], axis=0)
    tv = tv + shifted_y - unit_y
    tv = tv + jnp.where(lane_iota(volume.shape) >= 1, ahead(unit_x, -1), 0.0) - unit_x
    return tv


def settle(ref, sem):
    pltpu.make_async_copy(ref, ref, sem).wait()


def step_kernel(
    n, ns, slots, chunks, image_in, weights, ids_in, offs_in, count, measured_in,
    out, residual,
    wbuf, turned_w, image, measured, tiled, ids, offs, meta, table, halo, mine, pieces_all, lone, lone_all,
    cuts, cuts_all, turned, target, signals, grad, parts,
    wsem, load_sem, sent, meta_recv, halo_recv, piece_recv, lone_recv, cut_recv, grad_recv,
):
    me = lax.axis_index("vox")
    layer = lax.axis_index("sen")
    voxels = weights.shape[3]
    rows, samples = measured.shape[1:]
    tiles = samples // LANES
    lines = min(rows, SB)
    strips = SB // lines
    per = max(rows // SB, 1)

    barrier = pltpu.get_barrier_semaphore()
    for step in range(1, n):
        pl.semaphore_signal(barrier, inc=1, device_id={"vox": peer(me, n, n - step)}, device_id_type=MESH)
    for step in range(1, ns):
        pl.semaphore_signal(barrier, inc=1, device_id={"sen": peer(layer, ns, ns - step)}, device_id_type=MESH)

    arguments = []
    pairs = ((ids_in, ids), (offs_in, offs), (image_in, image), (measured_in, measured))
    for i, (src, dst) in enumerate(pairs):
        load = pltpu.make_async_copy(src, dst, load_sem.at[i])
        load.start()
        arguments.append(load)
    loads = []
    for k in range(slots):
        depth = voxels // chunks[k]
        strips_of = []
        for q in range(chunks[k]):
            part = pl.ds(q * depth, depth)
            load = pltpu.make_async_copy(weights.at[0, 0, k, part], wbuf.at[k, part], wsem.at[sum(chunks[:k]) + q])
            load.start(priority=1)
            strips_of.append(load)
        loads.append(strips_of)

    mask = block_mask(SB * WIN)
    alive = jnp.full((SB, LANES), count[0, 0])
    left = lane_iota((SB, LANES)) < WIN
    at = lane_iota((HALF, LANES))
    meta[...] = jnp.zeros_like(meta)
    arguments[0].wait()
    arguments[1].wait()
    meta[0:1, 0:slots] = ids[0]
    meta[1:2, 0:slots] = offs[0]
    pl.semaphore_wait(barrier, n - 1 + ns - 1)

    def remote(src, dst, send, recv, axis, to):
        pltpu.make_async_remote_copy(
            src_ref=src, dst_ref=dst, send_sem=send, recv_sem=recv,
            device_id={axis: to}, device_id_type=MESH,
        ).start()

    for step in range(1, n):
        remote(meta, table.at[me], sent, meta_recv, "vox", peer(me, n, n - step))
    pltpu.make_async_copy(meta, table.at[me], meta_recv).start()
    arguments[2].wait()
    for side, to in ((0, (me + 1) % n), (1, (me + n - 1) % n)):
        remote(image.at[0], halo.at[side], sent, halo_recv, "vox", to)
    low = image[0].astype(jnp.bfloat16)
    flat = jnp.concatenate([low[r : r + 1] for r in range(low.shape[0])], axis=1)
    flat = jnp.broadcast_to(flat, (SB, voxels))
    arguments[3].wait()
    for i in range(per * tiles):
        tiled[i] = measured[0, i // tiles * SB : i // tiles * SB + lines, i % tiles * LANES : (i % tiles + 1) * LANES]

    def forward(k):
        total = jnp.zeros((SB, SB * WIN), jnp.float32)
        depth = voxels // chunks[k]
        for q in range(chunks[k]):
            loads[k][q].wait()
            total = total + jnp.dot(
                flat[:, q * depth : (q + 1) * depth],
                wbuf[k, q * depth : (q + 1) * depth],
                preferred_element_type=jnp.float32,
            )
        total = jnp.where(mask, total, 0.0)
        tile = total[:, 0:LANES]
        for g in range(1, SB * WIN // LANES):
            tile = tile + total[:, g * LANES : (g + 1) * LANES]
        tile = tile + pltpu.roll(tile, WIN, 1)
        return jnp.where(alive > k, tile, 0.0)

    def spread_out(src, dst, recv):
        for step in range(1, n):
            remote(src, dst, sent, recv, "vox", peer(me, n, n - step))
        pltpu.make_async_copy(src, dst, recv).start()

    first = None
    for k in range(slots):
        tile = forward(k)
        if k % 2 == 1:
            mine[k // 2] = jnp.where(left, first, tile)
            spread_out(mine.at[k // 2], pieces_all.at[k // 2, me], piece_recv.at[k // 2])
        elif k == slots - 1:
            lone[...] = jnp.where(left[0:HALF], tile[0:HALF], tile[HALF:SB])
            spread_out(lone, lone_all.at[me], lone_recv)
        first = tile

    settle(table, meta_recv)

    def cut(j):
        across = lane_iota((lines, LANES))
        spans = []
        for k in range(slots):
            near = jnp.clip(table[j, 0, k] - me * per, 0, per - 1) * tiles
            start = table[j, 1, k]
            base = jnp.maximum(start - EDGE, 0)
            first = base // LANES
            after = jnp.minimum(first + 1, tiles - 1)
            one = tiled[near + first].astype(jnp.float32)
            two = tiled[near + after].astype(jnp.float32)
            span = jnp.where(across >= base % LANES, one, two)
            spans.append(pltpu.roll(span, (k * SPAN + EDGE - start) & (LANES - 1), 1))
        for i in range(cuts.shape[1]):
            packed = None
            for k in range(slots):
                begin = k * SPAN - i * LANES
                if begin + SPAN <= 0 or begin >= LANES:
                    continue
                packed = spans[k] if packed is None else jnp.where(across >= begin, spans[k], packed)
            cuts[j, i] = packed.astype(cuts.dtype)

    order = [peer(me, n, step) for step in range(n - 1, 0, -1)]
    for some in (order[:2], order[2:]):
        for to in some:
            cut(to)
        for to in some:
            remote(cuts.at[to], cuts_all.at[me], sent, cut_recv, "vox", to)
    cut(me)
    pltpu.make_async_copy(cuts.at[me], cuts_all.at[me], cut_recv).start()

    for k in range(slots):
        turned_w[k] = wbuf[k].T

    numbers = [table[me, 0, k] for k in range(slots)]
    starts = [table[me, 1, k] for k in range(slots)]
    times = [start - WIN // 2 + ((at - start + WIN // 2) & (LANES - 1)) for start in starts]
    keys = [number * FAR + time for number, time in zip(numbers, times)]
    lane = lane_iota((1, LANES))

    sums = (jnp.zeros((HALF, LANES), jnp.float32),) * (slots * 2)
    def gather(j, sums, ks, load):
        sums = list(sums)
        for k in ks:
            number, start = table[j, 0, k], table[j, 1, k]
            piece = load(j, k, start)
            turned[j, k] = piece
            since = (lane - start) & (LANES - 1)
            spot = number * tiles + lax.shift_right_logical(since + start, 7)
            target[j, k : k + 1] = jnp.where(since < WIN, spot, -1)
            key = number * FAR + start
            for i in range(slots):
                since = keys[i] - key
                inside = (since >= 0) & (since < WIN)
                for h in range(2):
                    part = piece[h * HALF : (h + 1) * HALF]
                    sums[2 * i + h] = sums[2 * i + h] + jnp.where(inside, part, 0.0)
        return tuple(sums)

    def load_pair(j, k, start):
        return pltpu.roll(pieces_all[k // 2, j], (start + (k % 2) * WIN) & (LANES - 1), 1)

    def load_lone(j, k, start):
        upper = pltpu.roll(lone_all[j], start & (LANES - 1), 1)
        lower = pltpu.roll(lone_all[j], (start + WIN) & (LANES - 1), 1)
        return jnp.concatenate([upper, lower], axis=0)

    for g in range(slots // 2):
        settle(pieces_all.at[g], piece_recv.at[g])
        sums = each(n, functools.partial(gather, ks=(2 * g, 2 * g + 1), load=load_pair), sums)
    if slots % 2:
        settle(lone_all, lone_recv)
        sums = each(n, functools.partial(gather, ks=(slots - 1,), load=load_lone), sums)

    derived = []
    for k in range(slots):
        value = jnp.concatenate([stencil(sums[2 * k]), stencil(sums[2 * k + 1])], axis=0)
        derived.append(pltpu.roll(value, (LANES + EDGE - starts[k]) & (LANES - 1), 1))
    wide = lane_iota((SB, LANES))
    settle(cuts_all, cut_recv)
    spreads = []
    for k in range(slots):
        stripes = []
        for i in range(strips):
            owner = numbers[k] * SB // rows + i
            begin, last = k * SPAN, (k + 1) * SPAN - 1
            stripe = cuts_all[owner, begin // LANES].astype(jnp.float32)
            if last // LANES > begin // LANES:
                follow = cuts_all[owner, last // LANES].astype(jnp.float32)
                stripe = jnp.where(lane_iota((lines, LANES)) >= begin % LANES, stripe, follow)
            stripes.append(stripe)
        block = stripes[0] if strips == 1 else jnp.concatenate(stripes, axis=0)
        if k:
            block = pltpu.roll(block, (-k * SPAN) % LANES, 1)
        time = wide + (starts[k] - EDGE)
        keep = (time >= 0) & (time < samples) & (jnp.full((SB, LANES), count[0, 0]) > k)
        window = -stencil(jnp.where(keep, derived[k] - block, 0.0))
        window = jnp.where(left, ahead(window, EDGE), ahead(window, EDGE - WIN))
        spread = jnp.concatenate([window] * (SB * WIN // LANES), axis=1)
        spreads.append(jnp.where(mask, spread, 0.0).astype(jnp.bfloat16))
    part = None
    for k in range(slots):
        term = jnp.dot(spreads[k], turned_w[k], preferred_element_type=jnp.float32)
        part = term if part is None else part + term
    grad[...] = jnp.sum(part, axis=0, keepdims=True)
    for step in range(ns - 1, 0, -1):
        remote(grad, parts.at[layer], sent, grad_recv, "sen", peer(layer, ns, step))
    pltpu.make_async_copy(grad, parts.at[layer], grad_recv).start()

    home = me * rows // SB * tiles

    def fill(i, carry):
        wanted = home + i

        def add(j, sums):
            low, high = sums
            for k in range(slots):
                here = jnp.broadcast_to(target[j, k : k + 1], (HALF, LANES)) == wanted
                low = low + jnp.where(here, turned[j, k, 0:HALF], 0.0)
                high = high + jnp.where(here, turned[j, k, HALF:SB], 0.0)
            return low, high

        low, high = each(n, add, (jnp.zeros((HALF, LANES), jnp.float32),) * 2)
        line = i // tiles * SB
        column = pl.ds(pl.multiple_of(i % tiles * LANES, LANES), LANES)
        signals[pl.ds(pl.multiple_of(line, SB), HALF), column] = low
        signals[pl.ds(pl.multiple_of(line + HALF, HALF), HALF), column] = high
        return carry

    lax.fori_loop(0, per * tiles, fill, 0)

    for r in range(0, rows, HALF):
        line = r if rows >= SB else pl.multiple_of((me * rows + r) % SB // HALF * HALF, HALF)
        block = stencil_edges(signals[pl.ds(line, HALF)])
        if rows % HALF == 0:
            residual[0, r : r + HALF] = block - measured[0, r : r + HALF].astype(jnp.float32)
        else:
            which = jnp.full((rows, samples), (me * rows) % HALF)
            own = block[0:rows]
            for i in range(1, HALF // rows):
                own = jnp.where(which == i * rows, block[i * rows : (i + 1) * rows], own)
            residual[0] = own - measured[0].astype(jnp.float32)

    settle(halo, halo_recv)
    tv = variation(n, me, image, halo)
    settle(table.at[pl.ds(0, n - 1)], sent)
    settle(halo, sent)
    settle(pieces_all.at[:, pl.ds(0, n - 1)], sent)
    if slots % 2:
        settle(lone_all.at[pl.ds(0, n - 1)], sent)
    settle(cuts_all.at[pl.ds(0, n - 1)], sent)
    settle(parts, grad_recv)
    flat = parts[0]
    for index in range(1, ns):
        flat = flat + parts[index]
    volume = image[0]
    width = volume.shape[1]
    for r in range(volume.shape[0]):
        total = flat[:, r * width : (r + 1) * width]
        out[0, r : r + 1] = volume[r : r + 1] - STEP_SIZE * (total + TV_WEIGHT * tv[r : r + 1])
    settle(parts.at[pl.ds(0, ns - 1)], sent)


def store_kernel(image, residual, image_out, residual_out, sem):
    rows = residual.shape[1]
    depth = rows // STORES if rows % (STORES * HALF) == 0 else rows
    copies = [pltpu.make_async_copy(image, image_out, sem.at[0])]
    for i, r in enumerate(range(0, rows, depth)):
        part = pl.ds(r, depth)
        copies.append(pltpu.make_async_copy(residual.at[:, part], residual_out.at[:, part], sem.at[1 + i]))
    for copy in copies:
        copy.start()
    for copy in copies:
        copy.wait()


def on_device(image, weights, block_ids, offsets, counts, measured):
    n = lax.axis_size("vox")
    ns = lax.axis_size("sen")
    slots, voxels, cells = weights.shape[2:]
    rows, samples = measured.shape[1:]
    pairs = slots // 2
    lines = min(rows, SB)
    chunks = (1,) * (slots - 1) + (4,)
    vmem = pl.BlockSpec(memory_space=pltpu.VMEM)
    hbm = pl.BlockSpec(memory_space=pltpu.HBM)
    smem = pl.BlockSpec(memory_space=pltpu.SMEM)
    dma = pltpu.SemaphoreType.DMA
    shape = jax.ShapeDtypeStruct

    def pin(value):
        return pltpu.with_memory_space_constraint(value, pltpu.HBM)

    image_next, residual = pl.pallas_call(
        functools.partial(step_kernel, n, ns, slots, chunks),
        out_shape=(shape(image.shape, jnp.float32), shape(measured.shape, jnp.float32)),
        in_specs=[hbm] * 4 + [smem, hbm],
        out_specs=(vmem, vmem),
        scratch_shapes=[
            pltpu.VMEM((slots, voxels, cells), jnp.bfloat16),
            pltpu.VMEM((slots, cells, voxels), jnp.bfloat16),
            pltpu.VMEM(image.shape, jnp.float32),
            pltpu.VMEM(measured.shape, measured.dtype),
            pltpu.VMEM((max(rows // SB, 1) * (samples // LANES), lines, LANES), jnp.bfloat16),
            pltpu.VMEM(block_ids.shape, jnp.int32),
            pltpu.VMEM(offsets.shape, jnp.int32),
            pltpu.VMEM((2, LANES), jnp.int32),
            pltpu.SMEM((n, 2, LANES), jnp.int32),
            pltpu.VMEM((2,) + image.shape[1:], jnp.float32),
            pltpu.VMEM((pairs, SB, LANES), jnp.float32),
            pltpu.VMEM((pairs, n, SB, LANES), jnp.float32),
            pltpu.VMEM((HALF, LANES), jnp.float32),
            pltpu.VMEM((n, HALF, LANES), jnp.float32),
            pltpu.VMEM((n, pl.cdiv(slots * SPAN, LANES), lines, LANES), jnp.bfloat16),
            pltpu.VMEM((n, pl.cdiv(slots * SPAN, LANES), lines, LANES), jnp.bfloat16),
            pltpu.VMEM((n, slots, SB, LANES), jnp.float32),
            pltpu.VMEM((n, HALF, LANES), jnp.int32),
            pltpu.VMEM((max(rows, SB), samples), jnp.float32),
            pltpu.VMEM((1, voxels), jnp.float32),
            pltpu.VMEM((ns, 1, voxels), jnp.float32),
            dma((sum(chunks),)),
            dma((4,)),
            dma,
            dma,
            dma,
            dma((pairs,)),
            dma,
            dma,
            dma,
        ],
        compiler_params=pltpu.CompilerParams(
            collective_id=0, has_side_effects=True, vmem_limit_bytes=40 << 20
        ),
        name="step_kernel",
    )(pin(image), pin(weights), pin(block_ids), pin(offsets), counts, pin(measured))

    return pl.pallas_call(
        store_kernel,
        out_shape=(shape(image.shape, jnp.float32), shape(measured.shape, jnp.float32)),
        in_specs=[vmem, vmem],
        out_specs=(hbm, hbm),
        scratch_shapes=[dma((1 + STORES,))],
        compiler_params=pltpu.CompilerParams(vmem_limit_bytes=1 << 20),
        name="store_kernel",
    )(image_next, residual)


def solution(mesh):
    placed = (
        P("vox", None, None),
        P("vox", "sen", None, None, None),
        P("vox", "sen", None),
        P("vox", "sen", None),
        P("vox", "sen"),
        P("sen", "vox", None),
    )
    return jax.shard_map(
        on_device,
        mesh=mesh,
        in_specs=placed,
        out_specs=(P("vox", None, None), P("sen", "vox", None)),
        check_vma=False,
    )
```

```python
import functools

import jax
import jax.numpy as jnp
from jax import lax
from jax.experimental import pallas as pl
from jax.experimental.pallas import tpu as pltpu
from jax.sharding import PartitionSpec as P

SB = 16
WIN = 64
LANES = 128
HALF = 8
EDGE = 2
SPAN = WIN + 2 * EDGE
FAR = 1 << 16
UNROLL = 8
EARLY = 2
STORES = 4

STEP_SIZE = 0.25
TV_WEIGHT = 0.3
TV_EPS = 0.01
C1 = 8.0 / 12.0
C2 = 1.0 / 12.0
MESH = pl.DeviceIdType.MESH


def lane_iota(shape):
    return lax.broadcasted_iota(jnp.int32, shape, len(shape) - 1)


def ahead(value, shift):
    length = value.shape[-1]
    return pltpu.roll(value, (-shift) % length, value.ndim - 1)


def stencil(value):
    return C2 * ahead(value, -2) - C1 * ahead(value, -1) + C1 * ahead(value, 1) - C2 * ahead(value, 2)


def stencil_edges(value):
    length = value.shape[-1]
    at = lane_iota(value.shape)
    total = jnp.where(at >= 2, C2 * ahead(value, -2), 0.0)
    total = total - jnp.where(at >= 1, C1 * ahead(value, -1), 0.0)
    total = total + jnp.where(at < length - 1, C1 * ahead(value, 1), 0.0)
    return total - jnp.where(at < length - 2, C2 * ahead(value, 2), 0.0)


def block_mask(width):
    row = lax.broadcasted_iota(jnp.int32, (SB, width), 0)
    return lane_iota((SB, width)) // WIN == row


def peer(me, count, i):
    return i + (i + count - me) // count


def each(count, body, carry):
    if count > UNROLL:
        return lax.fori_loop(0, count, body, carry)
    for i in range(count):
        carry = body(i, carry)
    return carry


def variation(n, place, image, halo):
    def units(volume, step_z):
        shape = volume.shape
        row = lax.broadcasted_iota(jnp.int32, shape, 0)
        below = jnp.concatenate([volume[1:], volume[shape[0] - 1 :]], axis=0)
        step_y = below - volume
        step_x = jnp.where(lane_iota(shape) < shape[1] - 1, ahead(volume, 1) - volume, 0.0)
        size = jnp.sqrt(step_z * step_z + step_y * step_y + step_x * step_x + TV_EPS)
        return step_z / size, step_y / size, step_x / size, row

    volume = image[0]
    before, after = halo[0], halo[1]
    is_first = jnp.full(volume.shape, place) == 0
    is_last = jnp.full(volume.shape, place) == n - 1
    lower_z, _, _, _ = units(before, volume - before)
    unit_z, unit_y, unit_x, row = units(volume, jnp.where(is_last, 0.0, after - volume))
    tv = jnp.where(is_first, 0.0, lower_z) - unit_z
    shifted_y = jnp.concatenate([jnp.zeros_like(unit_y[0:1]), unit_y[: unit_y.shape[0] - 1]], axis=0)
    tv = tv + shifted_y - unit_y
    tv = tv + jnp.where(lane_iota(volume.shape) >= 1, ahead(unit_x, -1), 0.0) - unit_x
    return tv


def settle(ref, sem):
    pltpu.make_async_copy(ref, ref, sem).wait()


def step_kernel(
    n, ns, slots, chunks, image_in, weights, ids_in, offs_in, count, measured_in,
    out, residual,
    wbuf, turned_w, image, measured, tiled, ids, offs, meta, table, halo, mine, pieces_all, lone, lone_all,
    cuts, cuts_all, turned, target, signals, grad, parts,
    wsem, load_sem, sent, meta_recv, halo_recv, piece_recv, lone_recv, cut_recv, grad_recv,
):
    me = lax.axis_index("vox")
    layer = lax.axis_index("sen")
    voxels = weights.shape[3]
    rows, samples = measured.shape[1:]
    tiles = samples // LANES
    lines = min(rows, SB)
    strips = SB // lines
    per = max(rows // SB, 1)

    barrier = pltpu.get_barrier_semaphore()
    for i in range(n - 1):
        pl.semaphore_signal(barrier, inc=1, device_id={"vox": peer(me, n, i)}, device_id_type=MESH)
    for i in range(ns - 1):
        pl.semaphore_signal(barrier, inc=1, device_id={"sen": peer(layer, ns, i)}, device_id_type=MESH)

    arguments = []
    pairs = ((ids_in, ids), (offs_in, offs), (image_in, image), (measured_in, measured))
    for i, (src, dst) in enumerate(pairs):
        load = pltpu.make_async_copy(src, dst, load_sem.at[i])
        load.start()
        arguments.append(load)
    loads = []
    for k in range(slots):
        depth = voxels // chunks[k]
        strips_of = []
        for q in range(chunks[k]):
            part = pl.ds(q * depth, depth)
            load = pltpu.make_async_copy(weights.at[0, 0, k, part], wbuf.at[k, part], wsem.at[sum(chunks[:k]) + q])
            load.start(priority=1)
            strips_of.append(load)
        loads.append(strips_of)

    mask = block_mask(SB * WIN)
    alive = jnp.full((SB, LANES), count[0, 0])
    left = lane_iota((SB, LANES)) < WIN
    at = lane_iota((HALF, LANES))
    meta[...] = jnp.zeros_like(meta)
    arguments[0].wait()
    arguments[1].wait()
    meta[0:1, 0:slots] = ids[0]
    meta[1:2, 0:slots] = offs[0]
    pl.semaphore_wait(barrier, n - 1 + ns - 1)

    def remote(src, dst, send, recv, axis, to):
        pltpu.make_async_remote_copy(
            src_ref=src, dst_ref=dst, send_sem=send, recv_sem=recv,
            device_id={axis: to}, device_id_type=MESH,
        ).start()

    for i in range(n - 1):
        remote(meta, table.at[me], sent, meta_recv, "vox", peer(me, n, i))
    pltpu.make_async_copy(meta, table.at[me], meta_recv).start()
    arguments[2].wait()
    for side, to in ((0, (me + 1) % n), (1, (me + n - 1) % n)):
        remote(image.at[0], halo.at[side], sent, halo_recv, "vox", to)
    low = image[0].astype(jnp.bfloat16)
    flat = jnp.concatenate([low[r : r + 1] for r in range(low.shape[0])], axis=1)
    flat = jnp.broadcast_to(flat, (SB, voxels))
    arguments[3].wait()
    for i in range(per * tiles):
        tiled[i] = measured[0, i // tiles * SB : i // tiles * SB + lines, i % tiles * LANES : (i % tiles + 1) * LANES]

    def forward(k):
        total = jnp.zeros((SB, SB * WIN), jnp.float32)
        depth = voxels // chunks[k]
        for q in range(chunks[k]):
            loads[k][q].wait()
            total = total + jnp.dot(
                flat[:, q * depth : (q + 1) * depth],
                wbuf[k, q * depth : (q + 1) * depth],
                preferred_element_type=jnp.float32,
            )
        total = jnp.where(mask, total, 0.0)
        tile = total[:, 0:LANES]
        for g in range(1, SB * WIN // LANES):
            tile = tile + total[:, g * LANES : (g + 1) * LANES]
        tile = tile + pltpu.roll(tile, WIN, 1)
        return jnp.where(alive > k, tile, 0.0)

    def spread_out(src, dst, recv):
        for i in range(n - 1):
            remote(src, dst, sent, recv, "vox", peer(me, n, i))
        pltpu.make_async_copy(src, dst, recv).start()

    first = None
    for k in range(slots):
        tile = forward(k)
        if k % 2 == 1:
            mine[k // 2] = jnp.where(left, first, tile)
            spread_out(mine.at[k // 2], pieces_all.at[k // 2, me], piece_recv.at[k // 2])
        elif k == slots - 1:
            lone[...] = jnp.where(left[0:HALF], tile[0:HALF], tile[HALF:SB])
            spread_out(lone, lone_all.at[me], lone_recv)
        first = tile

    def transpose(ks):
        for k in ks:
            turned_w[k] = wbuf[k].T

    early = range(min(EARLY, slots))

    @pl.when(me < n // 4)
    def _():
        transpose(early)

    settle(table, meta_recv)

    def cut(j):
        across = lane_iota((lines, LANES))
        spans = []
        for k in range(slots):
            near = jnp.clip(table[j, 0, k] - me * per, 0, per - 1) * tiles
            start = table[j, 1, k]
            base = jnp.maximum(start - EDGE, 0)
            first = base // LANES
            after = jnp.minimum(first + 1, tiles - 1)
            one = tiled[near + first].astype(jnp.float32)
            two = tiled[near + after].astype(jnp.float32)
            span = jnp.where(across >= base % LANES, one, two)
            spans.append(pltpu.roll(span, (k * SPAN + EDGE - start) & (LANES - 1), 1))
        for i in range(cuts.shape[1]):
            packed = None
            for k in range(slots):
                begin = k * SPAN - i * LANES
                if begin + SPAN <= 0 or begin >= LANES:
                    continue
                packed = spans[k] if packed is None else jnp.where(across >= begin, spans[k], packed)
            cuts[j, i] = packed.astype(cuts.dtype)

    order = [peer(me, n, i) for i in range(n - 1)]
    for some in (order[:1], order[1:]):
        for to in some:
            cut(to)
        for to in some:
            remote(cuts.at[to], cuts_all.at[me], sent, cut_recv, "vox", to)
    cut(me)
    pltpu.make_async_copy(cuts.at[me], cuts_all.at[me], cut_recv).start()

    @pl.when(me >= n // 4)
    def _():
        transpose(early)

    transpose(range(len(early), slots))

    numbers = [table[me, 0, k] for k in range(slots)]
    starts = [table[me, 1, k] for k in range(slots)]
    times = [start - WIN // 2 + ((at - start + WIN // 2) & (LANES - 1)) for start in starts]
    keys = [number * FAR + time for number, time in zip(numbers, times)]
    lane = lane_iota((1, LANES))

    sums = (jnp.zeros((HALF, LANES), jnp.float32),) * (slots * 2)
    def gather(j, sums, ks, load):
        sums = list(sums)
        for k in ks:
            number, start = table[j, 0, k], table[j, 1, k]
            piece = load(j, k, start)
            turned[j, k] = piece
            since = (lane - start) & (LANES - 1)
            spot = number * tiles + lax.shift_right_logical(since + start, 7)
            target[j, k : k + 1] = jnp.where(since < WIN, spot, -1)
            key = number * FAR + start
            for i in range(slots):
                since = keys[i] - key
                inside = (since >= 0) & (since < WIN)
                for h in range(2):
                    part = piece[h * HALF : (h + 1) * HALF]
                    sums[2 * i + h] = sums[2 * i + h] + jnp.where(inside, part, 0.0)
        return tuple(sums)

    def load_pair(j, k, start):
        return pltpu.roll(pieces_all[k // 2, j], (start + (k % 2) * WIN) & (LANES - 1), 1)

    def load_lone(j, k, start):
        upper = pltpu.roll(lone_all[j], start & (LANES - 1), 1)
        lower = pltpu.roll(lone_all[j], (start + WIN) & (LANES - 1), 1)
        return jnp.concatenate([upper, lower], axis=0)

    for g in range(slots // 2):
        settle(pieces_all.at[g], piece_recv.at[g])
        sums = each(n, functools.partial(gather, ks=(2 * g, 2 * g + 1), load=load_pair), sums)
    if slots % 2:
        settle(lone_all, lone_recv)
        sums = each(n, functools.partial(gather, ks=(slots - 1,), load=load_lone), sums)

    derived = []
    for k in range(slots):
        value = jnp.concatenate([stencil(sums[2 * k]), stencil(sums[2 * k + 1])], axis=0)
        derived.append(pltpu.roll(value, (k * SPAN + EDGE - starts[k]) & (LANES - 1), 1))
    wide = lane_iota((SB, LANES))
    settle(cuts_all, cut_recv)
    spreads = []
    for k in range(slots):
        stripes = []
        for i in range(strips):
            owner = numbers[k] * SB // rows + i
            begin, last = k * SPAN, (k + 1) * SPAN - 1
            stripe = cuts_all[owner, begin // LANES].astype(jnp.float32)
            if last // LANES > begin // LANES:
                follow = cuts_all[owner, last // LANES].astype(jnp.float32)
                stripe = jnp.where(lane_iota((lines, LANES)) >= begin % LANES, stripe, follow)
            stripes.append(stripe)
        block = stripes[0] if strips == 1 else jnp.concatenate(stripes, axis=0)
        time = ((wide - k * SPAN) & (LANES - 1)) + (starts[k] - EDGE)
        keep = (time >= 0) & (time < samples) & (jnp.full((SB, LANES), count[0, 0]) > k)
        window = -stencil(jnp.where(keep, derived[k] - block, 0.0))
        turn = k * SPAN + EDGE
        window = jnp.where(left, ahead(window, turn), ahead(window, turn - WIN))
        spread = jnp.concatenate([window] * (SB * WIN // LANES), axis=1)
        spreads.append(jnp.where(mask, spread, 0.0).astype(jnp.bfloat16))
    part = None
    for k in range(slots):
        term = jnp.dot(spreads[k], turned_w[k], preferred_element_type=jnp.float32)
        part = term if part is None else part + term
    grad[...] = jnp.sum(part, axis=0, keepdims=True)
    for i in range(ns - 1):
        remote(grad, parts.at[layer], sent, grad_recv, "sen", peer(layer, ns, i))
    pltpu.make_async_copy(grad, parts.at[layer], grad_recv).start()

    home = me * rows // SB * tiles

    def fill(i, carry):
        wanted = home + i

        def add(j, sums):
            low, high = sums
            for k in range(slots):
                here = jnp.broadcast_to(target[j, k : k + 1], (HALF, LANES)) == wanted
                low = low + jnp.where(here, turned[j, k, 0:HALF], 0.0)
                high = high + jnp.where(here, turned[j, k, HALF:SB], 0.0)
            return low, high

        low, high = each(n, add, (jnp.zeros((HALF, LANES), jnp.float32),) * 2)
        line = i // tiles * SB
        column = pl.ds(pl.multiple_of(i % tiles * LANES, LANES), LANES)
        signals[pl.ds(pl.multiple_of(line, SB), HALF), column] = low
        signals[pl.ds(pl.multiple_of(line + HALF, HALF), HALF), column] = high
        return carry

    lax.fori_loop(0, per * tiles, fill, 0)

    for r in range(0, rows, HALF):
        line = r if rows >= SB else pl.multiple_of((me * rows + r) % SB // HALF * HALF, HALF)
        block = stencil_edges(signals[pl.ds(line, HALF)])
        if rows % HALF == 0:
            residual[0, r : r + HALF] = block - measured[0, r : r + HALF].astype(jnp.float32)
        else:
            which = jnp.full((rows, samples), (me * rows) % HALF)
            own = block[0:rows]
            for i in range(1, HALF // rows):
                own = jnp.where(which == i * rows, block[i * rows : (i + 1) * rows], own)
            residual[0] = own - measured[0].astype(jnp.float32)

    settle(halo, halo_recv)
    tv = variation(n, me, image, halo)
    settle(table.at[pl.ds(0, n - 1)], sent)
    settle(halo, sent)
    settle(pieces_all.at[:, pl.ds(0, n - 1)], sent)
    if slots % 2:
        settle(lone_all.at[pl.ds(0, n - 1)], sent)
    settle(cuts_all.at[pl.ds(0, n - 1)], sent)
    settle(parts, grad_recv)
    flat = parts[0]
    for index in range(1, ns):
        flat = flat + parts[index]
    volume = image[0]
    width = volume.shape[1]
    for r in range(volume.shape[0]):
        total = flat[:, r * width : (r + 1) * width]
        out[0, r : r + 1] = volume[r : r + 1] - STEP_SIZE * (total + TV_WEIGHT * tv[r : r + 1])
    settle(parts.at[pl.ds(0, ns - 1)], sent)


def store_kernel(image, residual, image_out, residual_out, sem):
    rows = residual.shape[1]
    depth = rows // STORES if rows % (STORES * HALF) == 0 else rows
    copies = [pltpu.make_async_copy(image, image_out, sem.at[0])]
    for i, r in enumerate(range(0, rows, depth)):
        part = pl.ds(r, depth)
        copies.append(pltpu.make_async_copy(residual.at[:, part], residual_out.at[:, part], sem.at[1 + i]))
    for copy in copies:
        copy.start()
    for copy in copies:
        copy.wait()


def on_device(image, weights, block_ids, offsets, counts, measured):
    n = lax.axis_size("vox")
    ns = lax.axis_size("sen")
    slots, voxels, cells = weights.shape[2:]
    rows, samples = measured.shape[1:]
    pairs = slots // 2
    lines = min(rows, SB)
    chunks = (1,) * (slots - 1) + (4,)
    vmem = pl.BlockSpec(memory_space=pltpu.VMEM)
    hbm = pl.BlockSpec(memory_space=pltpu.HBM)
    smem = pl.BlockSpec(memory_space=pltpu.SMEM)
    dma = pltpu.SemaphoreType.DMA
    shape = jax.ShapeDtypeStruct

    def pin(value):
        return pltpu.with_memory_space_constraint(value, pltpu.HBM)

    image_next, residual = pl.pallas_call(
        functools.partial(step_kernel, n, ns, slots, chunks),
        out_shape=(shape(image.shape, jnp.float32), shape(measured.shape, jnp.float32)),
        in_specs=[hbm] * 4 + [smem, hbm],
        out_specs=(vmem, vmem),
        scratch_shapes=[
            pltpu.VMEM((slots, voxels, cells), jnp.bfloat16),
            pltpu.VMEM((slots, cells, voxels), jnp.bfloat16),
            pltpu.VMEM(image.shape, jnp.float32),
            pltpu.VMEM(measured.shape, measured.dtype),
            pltpu.VMEM((max(rows // SB, 1) * (samples // LANES), lines, LANES), jnp.bfloat16),
            pltpu.VMEM(block_ids.shape, jnp.int32),
            pltpu.VMEM(offsets.shape, jnp.int32),
            pltpu.VMEM((2, LANES), jnp.int32),
            pltpu.SMEM((n, 2, LANES), jnp.int32),
            pltpu.VMEM((2,) + image.shape[1:], jnp.float32),
            pltpu.VMEM((pairs, SB, LANES), jnp.float32),
            pltpu.VMEM((pairs, n, SB, LANES), jnp.float32),
            pltpu.VMEM((HALF, LANES), jnp.float32),
            pltpu.VMEM((n, HALF, LANES), jnp.float32),
            pltpu.VMEM((n, pl.cdiv(slots * SPAN, LANES), lines, LANES), jnp.bfloat16),
            pltpu.VMEM((n, pl.cdiv(slots * SPAN, LANES), lines, LANES), jnp.bfloat16),
            pltpu.VMEM((n, slots, SB, LANES), jnp.float32),
            pltpu.VMEM((n, HALF, LANES), jnp.int32),
            pltpu.VMEM((max(rows, SB), samples), jnp.float32),
            pltpu.VMEM((1, voxels), jnp.float32),
            pltpu.VMEM((ns, 1, voxels), jnp.float32),
            dma((sum(chunks),)),
            dma((4,)),
            dma,
            dma,
            dma,
            dma((pairs,)),
            dma,
            dma,
            dma,
        ],
        compiler_params=pltpu.CompilerParams(
            collective_id=0, has_side_effects=True, vmem_limit_bytes=40 << 20
        ),
        name="step_kernel",
    )(pin(image), pin(weights), pin(block_ids), pin(offsets), counts, pin(measured))

    return pl.pallas_call(
        store_kernel,
        out_shape=(shape(image.shape, jnp.float32), shape(measured.shape, jnp.float32)),
        in_specs=[vmem, vmem],
        out_specs=(hbm, hbm),
        scratch_shapes=[dma((1 + STORES,))],
        compiler_params=pltpu.CompilerParams(vmem_limit_bytes=1 << 20),
        name="store_kernel",
    )(image_next, residual)


def solution(mesh):
    placed = (
        P("vox", None, None),
        P("vox", "sen", None, None, None),
        P("vox", "sen", None),
        P("vox", "sen", None),
        P("vox", "sen"),
        P("sen", "vox", None),
    )
    return jax.shard_map(
        on_device,
        mesh=mesh,
        in_specs=placed,
        out_specs=(P("vox", None, None), P("sen", "vox", None)),
        check_vma=False,
    )
```

```python
import functools

import jax
import jax.numpy as jnp
from jax import lax
from jax.experimental import pallas as pl
from jax.experimental.pallas import tpu as pltpu
from jax.sharding import PartitionSpec as P

SB = 16
WIN = 64
LANES = 128
HALF = 8
EDGE = 2
SPAN = WIN + 2 * EDGE
FAR = 1 << 16
UNROLL = 8
EARLY = 2
STORES = 4

STEP_SIZE = 0.25
TV_WEIGHT = 0.3
TV_EPS = 0.01
C1 = 8.0 / 12.0
C2 = 1.0 / 12.0
MESH = pl.DeviceIdType.MESH


def lane_iota(shape):
    return lax.broadcasted_iota(jnp.int32, shape, len(shape) - 1)


def ahead(value, shift):
    length = value.shape[-1]
    return pltpu.roll(value, (-shift) % length, value.ndim - 1)


def stencil(value):
    return C2 * ahead(value, -2) - C1 * ahead(value, -1) + C1 * ahead(value, 1) - C2 * ahead(value, 2)


def stencil_edges(value):
    length = value.shape[-1]
    at = lane_iota(value.shape)
    total = jnp.where(at >= 2, C2 * ahead(value, -2), 0.0)
    total = total - jnp.where(at >= 1, C1 * ahead(value, -1), 0.0)
    total = total + jnp.where(at < length - 1, C1 * ahead(value, 1), 0.0)
    return total - jnp.where(at < length - 2, C2 * ahead(value, 2), 0.0)


def block_mask(width):
    row = lax.broadcasted_iota(jnp.int32, (SB, width), 0)
    return lane_iota((SB, width)) // WIN == row


def peer(me, count, i):
    return i + (i + count - me) // count


def each(count, body, carry):
    if count > UNROLL:
        return lax.fori_loop(0, count, body, carry)
    for i in range(count):
        carry = body(i, carry)
    return carry


def variation(n, place, image, halo):
    def units(volume, step_z):
        shape = volume.shape
        row = lax.broadcasted_iota(jnp.int32, shape, 0)
        below = jnp.concatenate([volume[1:], volume[shape[0] - 1 :]], axis=0)
        step_y = below - volume
        step_x = jnp.where(lane_iota(shape) < shape[1] - 1, ahead(volume, 1) - volume, 0.0)
        size = jnp.sqrt(step_z * step_z + step_y * step_y + step_x * step_x + TV_EPS)
        return step_z / size, step_y / size, step_x / size, row

    volume = image[0]
    before, after = halo[0], halo[1]
    is_first = jnp.full(volume.shape, place) == 0
    is_last = jnp.full(volume.shape, place) == n - 1
    lower_z, _, _, _ = units(before, volume - before)
    unit_z, unit_y, unit_x, row = units(volume, jnp.where(is_last, 0.0, after - volume))
    tv = jnp.where(is_first, 0.0, lower_z) - unit_z
    shifted_y = jnp.concatenate([jnp.zeros_like(unit_y[0:1]), unit_y[: unit_y.shape[0] - 1]], axis=0)
    tv = tv + shifted_y - unit_y
    tv = tv + jnp.where(lane_iota(volume.shape) >= 1, ahead(unit_x, -1), 0.0) - unit_x
    return tv


def settle(ref, sem):
    pltpu.make_async_copy(ref, ref, sem).wait()


def step_kernel(
    n, ns, slots, chunks, image_in, weights, ids_in, offs_in, count, measured_in,
    out, residual,
    wbuf, turned_w, image, measured, tiled, ids, offs, meta, table, halo, mine, pieces_all, lone, lone_all,
    cuts, cuts_all, turned, target, signals, grad, parts,
    wsem, load_sem, sent, meta_recv, halo_recv, piece_recv, lone_recv, cut_recv, grad_recv,
):
    me = lax.axis_index("vox")
    layer = lax.axis_index("sen")
    voxels = weights.shape[3]
    rows, samples = measured.shape[1:]
    tiles = samples // LANES
    lines = min(rows, SB)
    strips = SB // lines
    per = max(rows // SB, 1)

    barrier = pltpu.get_barrier_semaphore()
    for i in range(n - 1):
        pl.semaphore_signal(barrier, inc=1, device_id={"vox": peer(me, n, i)}, device_id_type=MESH)
    for i in range(ns - 1):
        pl.semaphore_signal(barrier, inc=1, device_id={"sen": peer(layer, ns, i)}, device_id_type=MESH)

    arguments = []
    pairs = ((ids_in, ids), (offs_in, offs), (image_in, image), (measured_in, measured))
    for i, (src, dst) in enumerate(pairs):
        load = pltpu.make_async_copy(src, dst, load_sem.at[i])
        load.start()
        arguments.append(load)
    loads = []
    for k in range(slots):
        depth = voxels // chunks[k]
        strips_of = []
        for q in range(chunks[k]):
            part = pl.ds(q * depth, depth)
            load = pltpu.make_async_copy(weights.at[0, 0, k, part], wbuf.at[k, part], wsem.at[sum(chunks[:k]) + q])
            load.start(priority=1)
            strips_of.append(load)
        loads.append(strips_of)

    mask = block_mask(SB * WIN)
    alive = jnp.full((SB, LANES), count[0, 0])
    left = lane_iota((SB, LANES)) < WIN
    at = lane_iota((HALF, LANES))
    meta[...] = jnp.zeros_like(meta)
    arguments[0].wait()
    arguments[1].wait()
    meta[0:1, 0:slots] = ids[0]
    meta[1:2, 0:slots] = offs[0]
    pl.semaphore_wait(barrier, n - 1 + ns - 1)

    def remote(src, dst, send, recv, axis, to):
        pltpu.make_async_remote_copy(
            src_ref=src, dst_ref=dst, send_sem=send, recv_sem=recv,
            device_id={axis: to}, device_id_type=MESH,
        ).start()

    for i in reversed(range(n - 1)):
        remote(meta, table.at[me], sent, meta_recv, "vox", peer(me, n, i))
    pltpu.make_async_copy(meta, table.at[me], meta_recv).start()
    arguments[2].wait()
    for side, to in ((0, (me + 1) % n), (1, (me + n - 1) % n)):
        remote(image.at[0], halo.at[side], sent, halo_recv, "vox", to)
    low = image[0].astype(jnp.bfloat16)
    flat = jnp.concatenate([low[r : r + 1] for r in range(low.shape[0])], axis=1)
    flat = jnp.broadcast_to(flat, (SB, voxels))
    arguments[3].wait()
    for i in range(per * tiles):
        tiled[i] = measured[0, i // tiles * SB : i // tiles * SB + lines, i % tiles * LANES : (i % tiles + 1) * LANES]

    def forward(k):
        total = jnp.zeros((SB, SB * WIN), jnp.float32)
        depth = voxels // chunks[k]
        for q in range(chunks[k]):
            loads[k][q].wait()
            total = total + jnp.dot(
                flat[:, q * depth : (q + 1) * depth],
                wbuf[k, q * depth : (q + 1) * depth],
                preferred_element_type=jnp.float32,
            )
        total = jnp.where(mask, total, 0.0)
        tile = total[:, 0:LANES]
        for g in range(1, SB * WIN // LANES):
            tile = tile + total[:, g * LANES : (g + 1) * LANES]
        tile = tile + pltpu.roll(tile, WIN, 1)
        return jnp.where(alive > k, tile, 0.0)

    def spread_out(src, dst, recv):
        for i in range(n - 1):
            remote(src, dst, sent, recv, "vox", peer(me, n, i))
        pltpu.make_async_copy(src, dst, recv).start()

    first = None
    for k in range(slots):
        tile = forward(k)
        if k % 2 == 1:
            mine[k // 2] = jnp.where(left, first, tile)
            spread_out(mine.at[k // 2], pieces_all.at[k // 2, me], piece_recv.at[k // 2])
        elif k == slots - 1:
            lone[...] = jnp.where(left[0:HALF], tile[0:HALF], tile[HALF:SB])
            spread_out(lone, lone_all.at[me], lone_recv)
        first = tile

    def transpose(ks):
        for k in ks:
            turned_w[k] = wbuf[k].T

    early = range(min(EARLY, slots))

    @pl.when(me < n // 4)
    def _():
        transpose(early)

    settle(table, meta_recv)

    def cut(j):
        across = lane_iota((lines, LANES))
        spans = []
        for k in range(slots):
            near = jnp.clip(table[j, 0, k] - me * per, 0, per - 1) * tiles
            start = table[j, 1, k]
            base = jnp.maximum(start - EDGE, 0)
            first = base // LANES
            after = jnp.minimum(first + 1, tiles - 1)
            one = tiled[near + first].astype(jnp.float32)
            two = tiled[near + after].astype(jnp.float32)
            span = jnp.where(across >= base % LANES, one, two)
            spans.append(pltpu.roll(span, (k * SPAN + EDGE - start) & (LANES - 1), 1))
        for i in range(cuts.shape[1]):
            packed = None
            for k in range(slots):
                begin = k * SPAN - i * LANES
                if begin + SPAN <= 0 or begin >= LANES:
                    continue
                packed = spans[k] if packed is None else jnp.where(across >= begin, spans[k], packed)
            cuts[j, i] = packed.astype(cuts.dtype)

    order = [peer(me, n, i) for i in range(n - 1)]
    for some in (order[:1], order[1:]):
        for to in some:
            cut(to)
        for to in some:
            remote(cuts.at[to], cuts_all.at[me], sent, cut_recv, "vox", to)
    cut(me)
    pltpu.make_async_copy(cuts.at[me], cuts_all.at[me], cut_recv).start()

    @pl.when(me >= n // 4)
    def _():
        transpose(early)

    transpose(range(len(early), slots))

    numbers = [table[me, 0, k] for k in range(slots)]
    starts = [table[me, 1, k] for k in range(slots)]
    times = [start - WIN // 2 + ((at - start + WIN // 2) & (LANES - 1)) for start in starts]
    keys = [number * FAR + time for number, time in zip(numbers, times)]
    lane = lane_iota((1, LANES))

    sums = (jnp.zeros((HALF, LANES), jnp.float32),) * (slots * 2)
    def gather(j, sums, ks, load):
        sums = list(sums)
        for k in ks:
            number, start = table[j, 0, k], table[j, 1, k]
            piece = load(j, k, start)
            turned[j, k] = piece
            since = (lane - start) & (LANES - 1)
            spot = number * tiles + lax.shift_right_logical(since + start, 7)
            target[j, k : k + 1] = jnp.where(since < WIN, spot, -1)
            key = number * FAR + start
            for i in range(slots):
                since = keys[i] - key
                inside = (since >= 0) & (since < WIN)
                for h in range(2):
                    part = piece[h * HALF : (h + 1) * HALF]
                    sums[2 * i + h] = sums[2 * i + h] + jnp.where(inside, part, 0.0)
        return tuple(sums)

    def load_pair(j, k, start):
        return pltpu.roll(pieces_all[k // 2, j], (start + (k % 2) * WIN) & (LANES - 1), 1)

    def load_lone(j, k, start):
        upper = pltpu.roll(lone_all[j], start & (LANES - 1), 1)
        lower = pltpu.roll(lone_all[j], (start + WIN) & (LANES - 1), 1)
        return jnp.concatenate([upper, lower], axis=0)

    for g in range(slots // 2):
        settle(pieces_all.at[g], piece_recv.at[g])
        sums = each(n, functools.partial(gather, ks=(2 * g, 2 * g + 1), load=load_pair), sums)
    if slots % 2:
        settle(lone_all, lone_recv)
        sums = each(n, functools.partial(gather, ks=(slots - 1,), load=load_lone), sums)

    derived = []
    for k in range(slots):
        value = jnp.concatenate([stencil(sums[2 * k]), stencil(sums[2 * k + 1])], axis=0)
        derived.append(pltpu.roll(value, (k * SPAN + EDGE - starts[k]) & (LANES - 1), 1))
    wide = lane_iota((SB, LANES))
    settle(cuts_all, cut_recv)
    spreads = []
    for k in range(slots):
        stripes = []
        for i in range(strips):
            owner = numbers[k] * SB // rows + i
            begin, last = k * SPAN, (k + 1) * SPAN - 1
            stripe = cuts_all[owner, begin // LANES].astype(jnp.float32)
            if last // LANES > begin // LANES:
                follow = cuts_all[owner, last // LANES].astype(jnp.float32)
                stripe = jnp.where(lane_iota((lines, LANES)) >= begin % LANES, stripe, follow)
            stripes.append(stripe)
        block = stripes[0] if strips == 1 else jnp.concatenate(stripes, axis=0)
        time = ((wide - k * SPAN) & (LANES - 1)) + (starts[k] - EDGE)
        keep = (time >= 0) & (time < samples) & (jnp.full((SB, LANES), count[0, 0]) > k)
        window = -stencil(jnp.where(keep, derived[k] - block, 0.0))
        turn = k * SPAN + EDGE
        window = jnp.where(left, ahead(window, turn), ahead(window, turn - WIN))
        spread = jnp.concatenate([window] * (SB * WIN // LANES), axis=1)
        spreads.append(jnp.where(mask, spread, 0.0).astype(jnp.bfloat16))
    part = None
    for k in range(slots):
        term = jnp.dot(spreads[k], turned_w[k], preferred_element_type=jnp.float32)
        part = term if part is None else part + term
    grad[...] = jnp.sum(part, axis=0, keepdims=True)
    for i in range(ns - 1):
        remote(grad, parts.at[layer], sent, grad_recv, "sen", peer(layer, ns, i))
    pltpu.make_async_copy(grad, parts.at[layer], grad_recv).start()

    home = me * rows // SB * tiles

    def fill(i, carry):
        wanted = home + i

        def add(j, sums):
            low, high = sums
            for k in range(slots):
                here = jnp.broadcast_to(target[j, k : k + 1], (HALF, LANES)) == wanted
                low = low + jnp.where(here, turned[j, k, 0:HALF], 0.0)
                high = high + jnp.where(here, turned[j, k, HALF:SB], 0.0)
            return low, high

        low, high = each(n, add, (jnp.zeros((HALF, LANES), jnp.float32),) * 2)
        line = i // tiles * SB
        column = pl.ds(pl.multiple_of(i % tiles * LANES, LANES), LANES)
        signals[pl.ds(pl.multiple_of(line, SB), HALF), column] = low
        signals[pl.ds(pl.multiple_of(line + HALF, HALF), HALF), column] = high
        return carry

    lax.fori_loop(0, per * tiles, fill, 0)

    for r in range(0, rows, HALF):
        line = r if rows >= SB else pl.multiple_of((me * rows + r) % SB // HALF * HALF, HALF)
        block = stencil_edges(signals[pl.ds(line, HALF)])
        if rows % HALF == 0:
            residual[0, r : r + HALF] = block - measured[0, r : r + HALF].astype(jnp.float32)
        else:
            which = jnp.full((rows, samples), (me * rows) % HALF)
            own = block[0:rows]
            for i in range(1, HALF // rows):
                own = jnp.where(which == i * rows, block[i * rows : (i + 1) * rows], own)
            residual[0] = own - measured[0].astype(jnp.float32)

    settle(halo, halo_recv)
    tv = variation(n, me, image, halo)
    settle(table.at[pl.ds(0, n - 1)], sent)
    settle(halo, sent)
    settle(pieces_all.at[:, pl.ds(0, n - 1)], sent)
    if slots % 2:
        settle(lone_all.at[pl.ds(0, n - 1)], sent)
    settle(cuts_all.at[pl.ds(0, n - 1)], sent)
    settle(parts, grad_recv)
    flat = parts[0]
    for index in range(1, ns):
        flat = flat + parts[index]
    volume = image[0]
    width = volume.shape[1]
    for r in range(volume.shape[0]):
        total = flat[:, r * width : (r + 1) * width]
        out[0, r : r + 1] = volume[r : r + 1] - STEP_SIZE * (total + TV_WEIGHT * tv[r : r + 1])
    settle(parts.at[pl.ds(0, ns - 1)], sent)


def store_kernel(image, residual, image_out, residual_out, sem):
    rows = residual.shape[1]
    depth = rows // STORES if rows % (STORES * HALF) == 0 else rows
    copies = [pltpu.make_async_copy(image, image_out, sem.at[0])]
    for i, r in enumerate(range(0, rows, depth)):
        part = pl.ds(r, depth)
        copies.append(pltpu.make_async_copy(residual.at[:, part], residual_out.at[:, part], sem.at[1 + i]))
    for copy in copies:
        copy.start()
    for copy in copies:
        copy.wait()


def on_device(image, weights, block_ids, offsets, counts, measured):
    n = lax.axis_size("vox")
    ns = lax.axis_size("sen")
    slots, voxels, cells = weights.shape[2:]
    rows, samples = measured.shape[1:]
    pairs = slots // 2
    lines = min(rows, SB)
    chunks = (1,) * (slots - 1) + (4,)
    vmem = pl.BlockSpec(memory_space=pltpu.VMEM)
    hbm = pl.BlockSpec(memory_space=pltpu.HBM)
    smem = pl.BlockSpec(memory_space=pltpu.SMEM)
    dma = pltpu.SemaphoreType.DMA
    shape = jax.ShapeDtypeStruct

    def pin(value):
        return pltpu.with_memory_space_constraint(value, pltpu.HBM)

    image_next, residual = pl.pallas_call(
        functools.partial(step_kernel, n, ns, slots, chunks),
        out_shape=(shape(image.shape, jnp.float32), shape(measured.shape, jnp.float32)),
        in_specs=[hbm] * 4 + [smem, hbm],
        out_specs=(vmem, vmem),
        scratch_shapes=[
            pltpu.VMEM((slots, voxels, cells), jnp.bfloat16),
            pltpu.VMEM((slots, cells, voxels), jnp.bfloat16),
            pltpu.VMEM(image.shape, jnp.float32),
            pltpu.VMEM(measured.shape, measured.dtype),
            pltpu.VMEM((max(rows // SB, 1) * (samples // LANES), lines, LANES), jnp.bfloat16),
            pltpu.VMEM(block_ids.shape, jnp.int32),
            pltpu.VMEM(offsets.shape, jnp.int32),
            pltpu.VMEM((2, LANES), jnp.int32),
            pltpu.SMEM((n, 2, LANES), jnp.int32),
            pltpu.VMEM((2,) + image.shape[1:], jnp.float32),
            pltpu.VMEM((pairs, SB, LANES), jnp.float32),
            pltpu.VMEM((pairs, n, SB, LANES), jnp.float32),
            pltpu.VMEM((HALF, LANES), jnp.float32),
            pltpu.VMEM((n, HALF, LANES), jnp.float32),
            pltpu.VMEM((n, pl.cdiv(slots * SPAN, LANES), lines, LANES), jnp.bfloat16),
            pltpu.VMEM((n, pl.cdiv(slots * SPAN, LANES), lines, LANES), jnp.bfloat16),
            pltpu.VMEM((n, slots, SB, LANES), jnp.float32),
            pltpu.VMEM((n, HALF, LANES), jnp.int32),
            pltpu.VMEM((max(rows, SB), samples), jnp.float32),
            pltpu.VMEM((1, voxels), jnp.float32),
            pltpu.VMEM((ns, 1, voxels), jnp.float32),
            dma((sum(chunks),)),
            dma((4,)),
            dma,
            dma,
            dma,
            dma((pairs,)),
            dma,
            dma,
            dma,
        ],
        compiler_params=pltpu.CompilerParams(
            collective_id=0, has_side_effects=True, vmem_limit_bytes=40 << 20
        ),
        name="step_kernel",
    )(pin(image), pin(weights), pin(block_ids), pin(offsets), counts, pin(measured))

    return pl.pallas_call(
        store_kernel,
        out_shape=(shape(image.shape, jnp.float32), shape(measured.shape, jnp.float32)),
        in_specs=[vmem, vmem],
        out_specs=(hbm, hbm),
        scratch_shapes=[dma((1 + STORES,))],
        compiler_params=pltpu.CompilerParams(vmem_limit_bytes=1 << 20),
        name="store_kernel",
    )(image_next, residual)


def solution(mesh):
    placed = (
        P("vox", None, None),
        P("vox", "sen", None, None, None),
        P("vox", "sen", None),
        P("vox", "sen", None),
        P("vox", "sen"),
        P("sen", "vox", None),
    )
    return jax.shard_map(
        on_device,
        mesh=mesh,
        in_specs=placed,
        out_specs=(P("vox", None, None), P("sen", "vox", None)),
        check_vma=False,
    )
```

```python
import functools

import jax
import jax.numpy as jnp
from jax import lax
from jax.experimental import pallas as pl
from jax.experimental.pallas import tpu as pltpu
from jax.sharding import PartitionSpec as P

SB = 16
WIN = 64
LANES = 128
HALF = 8
EDGE = 2
SPAN = WIN + 2 * EDGE
FAR = 1 << 16
UNROLL = 8
EARLY = 2
STORES = 1

STEP_SIZE = 0.25
TV_WEIGHT = 0.3
TV_EPS = 0.01
C1 = 8.0 / 12.0
C2 = 1.0 / 12.0
MESH = pl.DeviceIdType.MESH


def lane_iota(shape):
    return lax.broadcasted_iota(jnp.int32, shape, len(shape) - 1)


def ahead(value, shift):
    length = value.shape[-1]
    return pltpu.roll(value, (-shift) % length, value.ndim - 1)


def stencil(value):
    return C2 * ahead(value, -2) - C1 * ahead(value, -1) + C1 * ahead(value, 1) - C2 * ahead(value, 2)


def stencil_edges(value):
    length = value.shape[-1]
    at = lane_iota(value.shape)
    total = jnp.where(at >= 2, C2 * ahead(value, -2), 0.0)
    total = total - jnp.where(at >= 1, C1 * ahead(value, -1), 0.0)
    total = total + jnp.where(at < length - 1, C1 * ahead(value, 1), 0.0)
    return total - jnp.where(at < length - 2, C2 * ahead(value, 2), 0.0)


def block_mask(width):
    row = lax.broadcasted_iota(jnp.int32, (SB, width), 0)
    return lane_iota((SB, width)) // WIN == row


def peer(me, count, i):
    return i + (i + count - me) // count


def each(count, body, carry):
    if count > UNROLL:
        return lax.fori_loop(0, count, body, carry)
    for i in range(count):
        carry = body(i, carry)
    return carry


def variation(n, place, image, halo):
    def units(volume, step_z):
        shape = volume.shape
        row = lax.broadcasted_iota(jnp.int32, shape, 0)
        below = jnp.concatenate([volume[1:], volume[shape[0] - 1 :]], axis=0)
        step_y = below - volume
        step_x = jnp.where(lane_iota(shape) < shape[1] - 1, ahead(volume, 1) - volume, 0.0)
        size = jnp.sqrt(step_z * step_z + step_y * step_y + step_x * step_x + TV_EPS)
        return step_z / size, step_y / size, step_x / size, row

    volume = image[0]
    before, after = halo[0], halo[1]
    is_first = jnp.full(volume.shape, place) == 0
    is_last = jnp.full(volume.shape, place) == n - 1
    lower_z, _, _, _ = units(before, volume - before)
    unit_z, unit_y, unit_x, row = units(volume, jnp.where(is_last, 0.0, after - volume))
    tv = jnp.where(is_first, 0.0, lower_z) - unit_z
    shifted_y = jnp.concatenate([jnp.zeros_like(unit_y[0:1]), unit_y[: unit_y.shape[0] - 1]], axis=0)
    tv = tv + shifted_y - unit_y
    tv = tv + jnp.where(lane_iota(volume.shape) >= 1, ahead(unit_x, -1), 0.0) - unit_x
    return tv


def settle(ref, sem):
    pltpu.make_async_copy(ref, ref, sem).wait()


def step_kernel(
    n, ns, slots, chunks, image_in, weights, ids_in, offs_in, count, measured_in,
    out, residual,
    wbuf, turned_w, image, measured, tiled, ids, offs, meta, table, halo, mine, pieces_all, lone, lone_all,
    cuts, cuts_all, turned, target, signals, grad, parts,
    wsem, load_sem, sent, meta_recv, halo_recv, piece_recv, lone_recv, cut_recv, grad_recv,
):
    me = lax.axis_index("vox")
    layer = lax.axis_index("sen")
    voxels = weights.shape[3]
    rows, samples = measured.shape[1:]
    tiles = samples // LANES
    lines = min(rows, SB)
    strips = SB // lines
    per = max(rows // SB, 1)

    barrier = pltpu.get_barrier_semaphore()
    for i in range(n - 1):
        pl.semaphore_signal(barrier, inc=1, device_id={"vox": peer(me, n, i)}, device_id_type=MESH)
    for i in range(ns - 1):
        pl.semaphore_signal(barrier, inc=1, device_id={"sen": peer(layer, ns, i)}, device_id_type=MESH)

    arguments = []
    pairs = ((ids_in, ids), (offs_in, offs), (image_in, image), (measured_in, measured))
    for i, (src, dst) in enumerate(pairs):
        load = pltpu.make_async_copy(src, dst, load_sem.at[i])
        load.start()
        arguments.append(load)
    loads = []
    for k in range(slots):
        depth = voxels // chunks[k]
        strips_of = []
        for q in range(chunks[k]):
            part = pl.ds(q * depth, depth)
            load = pltpu.make_async_copy(weights.at[0, 0, k, part], wbuf.at[k, part], wsem.at[sum(chunks[:k]) + q])
            load.start(priority=1)
            strips_of.append(load)
        loads.append(strips_of)

    mask = block_mask(SB * WIN)
    alive = jnp.full((SB, LANES), count[0, 0])
    left = lane_iota((SB, LANES)) < WIN
    at = lane_iota((HALF, LANES))
    meta[...] = jnp.zeros_like(meta)
    arguments[0].wait()
    arguments[1].wait()
    meta[0:1, 0:slots] = ids[0]
    meta[1:2, 0:slots] = offs[0]
    pl.semaphore_wait(barrier, n - 1 + ns - 1)

    def remote(src, dst, send, recv, axis, to):
        pltpu.make_async_remote_copy(
            src_ref=src, dst_ref=dst, send_sem=send, recv_sem=recv,
            device_id={axis: to}, device_id_type=MESH,
        ).start()

    for i in reversed(range(n - 1)):
        remote(meta, table.at[me], sent, meta_recv, "vox", peer(me, n, i))
    pltpu.make_async_copy(meta, table.at[me], meta_recv).start()
    arguments[2].wait()
    for side, to in ((0, (me + 1) % n), (1, (me + n - 1) % n)):
        remote(image.at[0], halo.at[side], sent, halo_recv, "vox", to)
    low = image[0].astype(jnp.bfloat16)
    flat = jnp.concatenate([low[r : r + 1] for r in range(low.shape[0])], axis=1)
    flat = jnp.broadcast_to(flat, (SB, voxels))
    arguments[3].wait()
    for i in range(per * tiles):
        tiled[i] = measured[0, i // tiles * SB : i // tiles * SB + lines, i % tiles * LANES : (i % tiles + 1) * LANES]

    def forward(k):
        total = jnp.zeros((SB, SB * WIN), jnp.float32)
        depth = voxels // chunks[k]
        for q in range(chunks[k]):
            loads[k][q].wait()
            total = total + jnp.dot(
                flat[:, q * depth : (q + 1) * depth],
                wbuf[k, q * depth : (q + 1) * depth],
                preferred_element_type=jnp.float32,
            )
        total = jnp.where(mask, total, 0.0)
        tile = total[:, 0:LANES]
        for g in range(1, SB * WIN // LANES):
            tile = tile + total[:, g * LANES : (g + 1) * LANES]
        tile = tile + pltpu.roll(tile, WIN, 1)
        return jnp.where(alive > k, tile, 0.0)

    def spread_out(src, dst, recv):
        for i in range(n - 1):
            remote(src, dst, sent, recv, "vox", peer(me, n, i))
        pltpu.make_async_copy(src, dst, recv).start()

    first = None
    for k in range(slots):
        tile = forward(k)
        if k % 2 == 1:
            mine[k // 2] = jnp.where(left, first, tile)
            spread_out(mine.at[k // 2], pieces_all.at[k // 2, me], piece_recv.at[k // 2])
        elif k == slots - 1:
            lone[...] = jnp.where(left[0:HALF], tile[0:HALF], tile[HALF:SB])
            spread_out(lone, lone_all.at[me], lone_recv)
        first = tile

    def transpose(ks):
        for k in ks:
            turned_w[k] = wbuf[k].T

    early = range(min(EARLY, slots))

    @pl.when(me < n // 4)
    def _():
        transpose(early)

    settle(table, meta_recv)

    def cut(j):
        across = lane_iota((lines, LANES))
        spans = []
        for k in range(slots):
            near = jnp.clip(table[j, 0, k] - me * per, 0, per - 1) * tiles
            start = table[j, 1, k]
            base = jnp.maximum(start - EDGE, 0)
            first = base // LANES
            after = jnp.minimum(first + 1, tiles - 1)
            one = tiled[near + first].astype(jnp.float32)
            two = tiled[near + after].astype(jnp.float32)
            span = jnp.where(across >= base % LANES, one, two)
            spans.append(pltpu.roll(span, (k * SPAN + EDGE - start) & (LANES - 1), 1))
        for i in range(cuts.shape[1]):
            packed = None
            for k in range(slots):
                begin = k * SPAN - i * LANES
                if begin + SPAN <= 0 or begin >= LANES:
                    continue
                packed = spans[k] if packed is None else jnp.where(across >= begin, spans[k], packed)
            cuts[j, i] = packed.astype(cuts.dtype)

    order = [peer(me, n, i) for i in range(n - 1)]
    for some in (order[:1], order[1:]):
        for to in some:
            cut(to)
        for to in some:
            remote(cuts.at[to], cuts_all.at[me], sent, cut_recv, "vox", to)
    cut(me)
    pltpu.make_async_copy(cuts.at[me], cuts_all.at[me], cut_recv).start()

    @pl.when(me >= n // 4)
    def _():
        transpose(early)

    transpose(range(len(early), slots))

    numbers = [table[me, 0, k] for k in range(slots)]
    starts = [table[me, 1, k] for k in range(slots)]
    times = [start - WIN // 2 + ((at - start + WIN // 2) & (LANES - 1)) for start in starts]
    keys = [number * FAR + time for number, time in zip(numbers, times)]
    lane = lane_iota((1, LANES))

    sums = (jnp.zeros((HALF, LANES), jnp.float32),) * (slots * 2)
    def gather(j, sums, ks, load):
        sums = list(sums)
        for k in ks:
            number, start = table[j, 0, k], table[j, 1, k]
            piece = load(j, k, start)
            turned[j, k] = piece
            since = (lane - start) & (LANES - 1)
            spot = number * tiles + lax.shift_right_logical(since + start, 7)
            target[j, k : k + 1] = jnp.where(since < WIN, spot, -1)
            key = number * FAR + start
            for i in range(slots):
                since = keys[i] - key
                inside = (since >= 0) & (since < WIN)
                for h in range(2):
                    part = piece[h * HALF : (h + 1) * HALF]
                    sums[2 * i + h] = sums[2 * i + h] + jnp.where(inside, part, 0.0)
        return tuple(sums)

    def load_pair(j, k, start):
        return pltpu.roll(pieces_all[k // 2, j], (start + (k % 2) * WIN) & (LANES - 1), 1)

    def load_lone(j, k, start):
        upper = pltpu.roll(lone_all[j], start & (LANES - 1), 1)
        lower = pltpu.roll(lone_all[j], (start + WIN) & (LANES - 1), 1)
        return jnp.concatenate([upper, lower], axis=0)

    for g in range(slots // 2):
        settle(pieces_all.at[g], piece_recv.at[g])
        sums = each(n, functools.partial(gather, ks=(2 * g, 2 * g + 1), load=load_pair), sums)
    if slots % 2:
        settle(lone_all, lone_recv)
        sums = each(n, functools.partial(gather, ks=(slots - 1,), load=load_lone), sums)

    derived = []
    for k in range(slots):
        value = jnp.concatenate([stencil(sums[2 * k]), stencil(sums[2 * k + 1])], axis=0)
        derived.append(pltpu.roll(value, (k * SPAN + EDGE - starts[k]) & (LANES - 1), 1))
    wide = lane_iota((SB, LANES))
    settle(cuts_all, cut_recv)
    spreads = []
    for k in range(slots):
        stripes = []
        for i in range(strips):
            owner = numbers[k] * SB // rows + i
            begin, last = k * SPAN, (k + 1) * SPAN - 1
            stripe = cuts_all[owner, begin // LANES].astype(jnp.float32)
            if last // LANES > begin // LANES:
                follow = cuts_all[owner, last // LANES].astype(jnp.float32)
                stripe = jnp.where(lane_iota((lines, LANES)) >= begin % LANES, stripe, follow)
            stripes.append(stripe)
        block = stripes[0] if strips == 1 else jnp.concatenate(stripes, axis=0)
        time = ((wide - k * SPAN) & (LANES - 1)) + (starts[k] - EDGE)
        keep = (time >= 0) & (time < samples) & (jnp.full((SB, LANES), count[0, 0]) > k)
        window = -stencil(jnp.where(keep, derived[k] - block, 0.0))
        turn = k * SPAN + EDGE
        window = jnp.where(left, ahead(window, turn), ahead(window, turn - WIN))
        spread = jnp.concatenate([window] * (SB * WIN // LANES), axis=1)
        spreads.append(jnp.where(mask, spread, 0.0).astype(jnp.bfloat16))
    part = None
    for k in range(slots):
        term = jnp.dot(spreads[k], turned_w[k], preferred_element_type=jnp.float32)
        part = term if part is None else part + term
    grad[...] = jnp.sum(part, axis=0, keepdims=True)
    for i in range(ns - 1):
        remote(grad, parts.at[layer], sent, grad_recv, "sen", peer(layer, ns, i))
    pltpu.make_async_copy(grad, parts.at[layer], grad_recv).start()

    home = me * rows // SB * tiles

    def fill(i, carry):
        wanted = home + i

        def add(j, sums):
            low, high = sums
            for k in range(slots):
                here = jnp.broadcast_to(target[j, k : k + 1], (HALF, LANES)) == wanted
                low = low + jnp.where(here, turned[j, k, 0:HALF], 0.0)
                high = high + jnp.where(here, turned[j, k, HALF:SB], 0.0)
            return low, high

        low, high = each(n, add, (jnp.zeros((HALF, LANES), jnp.float32),) * 2)
        line = i // tiles * SB
        column = pl.ds(pl.multiple_of(i % tiles * LANES, LANES), LANES)
        signals[pl.ds(pl.multiple_of(line, SB), HALF), column] = low
        signals[pl.ds(pl.multiple_of(line + HALF, HALF), HALF), column] = high
        return carry

    lax.fori_loop(0, per * tiles, fill, 0)

    for r in range(0, rows, HALF):
        line = r if rows >= SB else pl.multiple_of((me * rows + r) % SB // HALF * HALF, HALF)
        block = stencil_edges(signals[pl.ds(line, HALF)])
        if rows % HALF == 0:
            residual[0, r : r + HALF] = block - measured[0, r : r + HALF].astype(jnp.float32)
        else:
            which = jnp.full((rows, samples), (me * rows) % HALF)
            own = block[0:rows]
            for i in range(1, HALF // rows):
                own = jnp.where(which == i * rows, block[i * rows : (i + 1) * rows], own)
            residual[0] = own - measured[0].astype(jnp.float32)

    settle(halo, halo_recv)
    tv = variation(n, me, image, halo)
    settle(table.at[pl.ds(0, n - 1)], sent)
    settle(halo, sent)
    settle(pieces_all.at[:, pl.ds(0, n - 1)], sent)
    if slots % 2:
        settle(lone_all.at[pl.ds(0, n - 1)], sent)
    settle(cuts_all.at[pl.ds(0, n - 1)], sent)
    settle(parts, grad_recv)
    flat = parts[0]
    for index in range(1, ns):
        flat = flat + parts[index]
    volume = image[0]
    width = volume.shape[1]
    for r in range(volume.shape[0]):
        total = flat[:, r * width : (r + 1) * width]
        out[0, r : r + 1] = volume[r : r + 1] - STEP_SIZE * (total + TV_WEIGHT * tv[r : r + 1])
    settle(parts.at[pl.ds(0, ns - 1)], sent)


def store_kernel(image, residual, image_out, residual_out, sem):
    rows = residual.shape[1]
    depth = rows // STORES if rows % (STORES * HALF) == 0 else rows
    copies = [pltpu.make_async_copy(image, image_out, sem.at[0])]
    for i, r in enumerate(range(0, rows, depth)):
        part = pl.ds(r, depth)
        copies.append(pltpu.make_async_copy(residual.at[:, part], residual_out.at[:, part], sem.at[1 + i]))
    for copy in copies:
        copy.start()
    for copy in copies:
        copy.wait()


def on_device(image, weights, block_ids, offsets, counts, measured):
    n = lax.axis_size("vox")
    ns = lax.axis_size("sen")
    slots, voxels, cells = weights.shape[2:]
    rows, samples = measured.shape[1:]
    pairs = slots // 2
    lines = min(rows, SB)
    chunks = (1,) * (slots - 1) + (2,)
    vmem = pl.BlockSpec(memory_space=pltpu.VMEM)
    hbm = pl.BlockSpec(memory_space=pltpu.HBM)
    smem = pl.BlockSpec(memory_space=pltpu.SMEM)
    dma = pltpu.SemaphoreType.DMA
    shape = jax.ShapeDtypeStruct

    def pin(value):
        return pltpu.with_memory_space_constraint(value, pltpu.HBM)

    image_next, residual = pl.pallas_call(
        functools.partial(step_kernel, n, ns, slots, chunks),
        out_shape=(shape(image.shape, jnp.float32), shape(measured.shape, jnp.float32)),
        in_specs=[hbm] * 4 + [smem, hbm],
        out_specs=(vmem, vmem),
        scratch_shapes=[
            pltpu.VMEM((slots, voxels, cells), jnp.bfloat16),
            pltpu.VMEM((slots, cells, voxels), jnp.bfloat16),
            pltpu.VMEM(image.shape, jnp.float32),
            pltpu.VMEM(measured.shape, measured.dtype),
            pltpu.VMEM((max(rows // SB, 1) * (samples // LANES), lines, LANES), jnp.bfloat16),
            pltpu.VMEM(block_ids.shape, jnp.int32),
            pltpu.VMEM(offsets.shape, jnp.int32),
            pltpu.VMEM((2, LANES), jnp.int32),
            pltpu.SMEM((n, 2, LANES), jnp.int32),
            pltpu.VMEM((2,) + image.shape[1:], jnp.float32),
            pltpu.VMEM((pairs, SB, LANES), jnp.float32),
            pltpu.VMEM((pairs, n, SB, LANES), jnp.float32),
            pltpu.VMEM((HALF, LANES), jnp.float32),
            pltpu.VMEM((n, HALF, LANES), jnp.float32),
            pltpu.VMEM((n, pl.cdiv(slots * SPAN, LANES), lines, LANES), jnp.bfloat16),
            pltpu.VMEM((n, pl.cdiv(slots * SPAN, LANES), lines, LANES), jnp.bfloat16),
            pltpu.VMEM((n, slots, SB, LANES), jnp.float32),
            pltpu.VMEM((n, HALF, LANES), jnp.int32),
            pltpu.VMEM((max(rows, SB), samples), jnp.float32),
            pltpu.VMEM((1, voxels), jnp.float32),
            pltpu.VMEM((ns, 1, voxels), jnp.float32),
            dma((sum(chunks),)),
            dma((4,)),
            dma,
            dma,
            dma,
            dma((pairs,)),
            dma,
            dma,
            dma,
        ],
        compiler_params=pltpu.CompilerParams(
            collective_id=0, has_side_effects=True, vmem_limit_bytes=40 << 20
        ),
        name="step_kernel",
    )(pin(image), pin(weights), pin(block_ids), pin(offsets), counts, pin(measured))

    return pl.pallas_call(
        store_kernel,
        out_shape=(shape(image.shape, jnp.float32), shape(measured.shape, jnp.float32)),
        in_specs=[vmem, vmem],
        out_specs=(hbm, hbm),
        scratch_shapes=[dma((1 + STORES,))],
        compiler_params=pltpu.CompilerParams(vmem_limit_bytes=1 << 20),
        name="store_kernel",
    )(image_next, residual)


def solution(mesh):
    placed = (
        P("vox", None, None),
        P("vox", "sen", None, None, None),
        P("vox", "sen", None),
        P("vox", "sen", None),
        P("vox", "sen"),
        P("sen", "vox", None),
    )
    return jax.shard_map(
        on_device,
        mesh=mesh,
        in_specs=placed,
        out_specs=(P("vox", None, None), P("sen", "vox", None)),
        check_vma=False,
    )
```

```python
import functools

import jax
import jax.numpy as jnp
from jax import lax
from jax.experimental import pallas as pl
from jax.experimental.pallas import tpu as pltpu
from jax.sharding import PartitionSpec as P

SB = 16
WIN = 64
LANES = 128
HALF = 8
EDGE = 2
SPAN = WIN + 2 * EDGE
FAR = 1 << 16
UNROLL = 8
EARLY = 2
STORES = 1

STEP_SIZE = 0.25
TV_WEIGHT = 0.3
TV_EPS = 0.01
C1 = 8.0 / 12.0
C2 = 1.0 / 12.0
MESH = pl.DeviceIdType.MESH


def lane_iota(shape):
    return lax.broadcasted_iota(jnp.int32, shape, len(shape) - 1)


def ahead(value, shift):
    length = value.shape[-1]
    return pltpu.roll(value, (-shift) % length, value.ndim - 1)


def stencil(value):
    return C2 * ahead(value, -2) - C1 * ahead(value, -1) + C1 * ahead(value, 1) - C2 * ahead(value, 2)


def stencil_edges(value):
    length = value.shape[-1]
    at = lane_iota(value.shape)
    total = jnp.where(at >= 2, C2 * ahead(value, -2), 0.0)
    total = total - jnp.where(at >= 1, C1 * ahead(value, -1), 0.0)
    total = total + jnp.where(at < length - 1, C1 * ahead(value, 1), 0.0)
    return total - jnp.where(at < length - 2, C2 * ahead(value, 2), 0.0)


def block_mask(width):
    row = lax.broadcasted_iota(jnp.int32, (SB, width), 0)
    return lane_iota((SB, width)) // WIN == row


def peer(me, count, i):
    return i + (i + count - me) // count


def each(count, body, carry):
    if count > UNROLL:
        return lax.fori_loop(0, count, body, carry)
    for i in range(count):
        carry = body(i, carry)
    return carry


def variation(n, place, image, halo):
    def units(volume, step_z):
        shape = volume.shape
        row = lax.broadcasted_iota(jnp.int32, shape, 0)
        below = jnp.concatenate([volume[1:], volume[shape[0] - 1 :]], axis=0)
        step_y = below - volume
        step_x = jnp.where(lane_iota(shape) < shape[1] - 1, ahead(volume, 1) - volume, 0.0)
        size = jnp.sqrt(step_z * step_z + step_y * step_y + step_x * step_x + TV_EPS)
        return step_z / size, step_y / size, step_x / size, row

    volume = image[0]
    before, after = halo[0], halo[1]
    is_first = jnp.full(volume.shape, place) == 0
    is_last = jnp.full(volume.shape, place) == n - 1
    lower_z, _, _, _ = units(before, volume - before)
    unit_z, unit_y, unit_x, row = units(volume, jnp.where(is_last, 0.0, after - volume))
    tv = jnp.where(is_first, 0.0, lower_z) - unit_z
    shifted_y = jnp.concatenate([jnp.zeros_like(unit_y[0:1]), unit_y[: unit_y.shape[0] - 1]], axis=0)
    tv = tv + shifted_y - unit_y
    tv = tv + jnp.where(lane_iota(volume.shape) >= 1, ahead(unit_x, -1), 0.0) - unit_x
    return tv


def settle(ref, sem):
    pltpu.make_async_copy(ref, ref, sem).wait()


def step_kernel(
    n, ns, slots, chunks, image_in, weights, ids_in, offs_in, count, measured_in,
    out, residual,
    wbuf, turned_w, image, measured, tiled, ids, offs, meta, table, halo, mine, pieces_all, lone, lone_all,
    cuts, cuts_all, turned, target, signals, grad, parts,
    wsem, load_sem, sent, meta_recv, halo_recv, piece_recv, lone_recv, cut_recv, grad_recv,
):
    me = lax.axis_index("vox")
    layer = lax.axis_index("sen")
    voxels = weights.shape[3]
    rows, samples = measured.shape[1:]
    tiles = samples // LANES
    lines = min(rows, SB)
    strips = SB // lines
    per = max(rows // SB, 1)

    barrier = pltpu.get_barrier_semaphore()
    for i in range(n - 1):
        pl.semaphore_signal(barrier, inc=1, device_id={"vox": peer(me, n, i)}, device_id_type=MESH)
    for i in range(ns - 1):
        pl.semaphore_signal(barrier, inc=1, device_id={"sen": peer(layer, ns, i)}, device_id_type=MESH)

    arguments = []
    pairs = ((ids_in, ids), (offs_in, offs), (image_in, image), (measured_in, measured))
    for i, (src, dst) in enumerate(pairs):
        load = pltpu.make_async_copy(src, dst, load_sem.at[i // 2])
        load.start()
        arguments.append(load)
    loads = []
    for k in range(slots):
        depth = voxels // chunks[k]
        strips_of = []
        for q in range(chunks[k]):
            part = pl.ds(q * depth, depth)
            load = pltpu.make_async_copy(weights.at[0, 0, k, part], wbuf.at[k, part], wsem.at[sum(chunks[:k]) + q])
            load.start(priority=1)
            strips_of.append(load)
        loads.append(strips_of)

    mask = block_mask(SB * WIN)
    alive = jnp.full((SB, LANES), count[0, 0])
    left = lane_iota((SB, LANES)) < WIN
    at = lane_iota((HALF, LANES))
    meta[...] = jnp.zeros_like(meta)
    arguments[0].wait()
    arguments[1].wait()
    meta[0:1, 0:slots] = ids[0]
    meta[1:2, 0:slots] = offs[0]
    pl.semaphore_wait(barrier, n - 1 + ns - 1)

    def remote(src, dst, send, recv, axis, to):
        pltpu.make_async_remote_copy(
            src_ref=src, dst_ref=dst, send_sem=send, recv_sem=recv,
            device_id={axis: to}, device_id_type=MESH,
        ).start()

    for i in reversed(range(n - 1)):
        remote(meta, table.at[me], sent, meta_recv, "vox", peer(me, n, i))
    pltpu.make_async_copy(meta, table.at[me], meta_recv).start()
    arguments[2].wait()
    arguments[3].wait()
    for side, to in ((0, (me + 1) % n), (1, (me + n - 1) % n)):
        remote(image.at[0], halo.at[side], sent, halo_recv, "vox", to)
    low = image[0].astype(jnp.bfloat16)
    flat = jnp.concatenate([low[r : r + 1] for r in range(low.shape[0])], axis=1)
    flat = jnp.broadcast_to(flat, (SB, voxels))
    for i in range(per * tiles):
        tiled[i] = measured[0, i // tiles * SB : i // tiles * SB + lines, i % tiles * LANES : (i % tiles + 1) * LANES]

    def forward(k):
        total = jnp.zeros((SB, SB * WIN), jnp.float32)
        depth = voxels // chunks[k]
        for q in range(chunks[k]):
            loads[k][q].wait()
            total = total + jnp.dot(
                flat[:, q * depth : (q + 1) * depth],
                wbuf[k, q * depth : (q + 1) * depth],
                preferred_element_type=jnp.float32,
            )
        total = jnp.where(mask, total, 0.0)
        tile = total[:, 0:LANES]
        for g in range(1, SB * WIN // LANES):
            tile = tile + total[:, g * LANES : (g + 1) * LANES]
        tile = tile + pltpu.roll(tile, WIN, 1)
        return jnp.where(alive > k, tile, 0.0)

    def spread_out(src, dst, recv):
        for i in range(n - 1):
            remote(src, dst, sent, recv, "vox", peer(me, n, i))
        pltpu.make_async_copy(src, dst, recv).start()

    first = None
    for k in range(slots):
        tile = forward(k)
        if k % 2 == 1:
            mine[k // 2] = jnp.where(left, first, tile)
            spread_out(mine.at[k // 2], pieces_all.at[k // 2, me], piece_recv.at[k // 2])
        elif k == slots - 1:
            lone[...] = jnp.where(left[0:HALF], tile[0:HALF], tile[HALF:SB])
            spread_out(lone, lone_all.at[me], lone_recv)
        first = tile

    def transpose(ks):
        for k in ks:
            turned_w[k] = wbuf[k].T

    early = range(min(EARLY, slots))

    @pl.when(me < n // 4)
    def _():
        transpose(early)

    settle(table, meta_recv)

    def cut(j):
        across = lane_iota((lines, LANES))
        spans = []
        for k in range(slots):
            near = jnp.clip(table[j, 0, k] - me * per, 0, per - 1) * tiles
            start = table[j, 1, k]
            base = jnp.maximum(start - EDGE, 0)
            first = base // LANES
            after = jnp.minimum(first + 1, tiles - 1)
            one = tiled[near + first].astype(jnp.float32)
            two = tiled[near + after].astype(jnp.float32)
            span = jnp.where(across >= base % LANES, one, two)
            spans.append(pltpu.roll(span, (k * SPAN + EDGE - start) & (LANES - 1), 1))
        for i in range(cuts.shape[1]):
            packed = None
            for k in range(slots):
                begin = k * SPAN - i * LANES
                if begin + SPAN <= 0 or begin >= LANES:
                    continue
                packed = spans[k] if packed is None else jnp.where(across >= begin, spans[k], packed)
            cuts[j, i] = packed.astype(cuts.dtype)

    order = [peer(me, n, i) for i in range(n - 1)]
    for some in (order[:1], order[1:]):
        for to in some:
            cut(to)
        for to in some:
            remote(cuts.at[to], cuts_all.at[me], sent, cut_recv, "vox", to)
    cut(me)
    pltpu.make_async_copy(cuts.at[me], cuts_all.at[me], cut_recv).start()

    @pl.when(me >= n // 4)
    def _():
        transpose(early)

    transpose(range(len(early), slots))

    numbers = [table[me, 0, k] for k in range(slots)]
    starts = [table[me, 1, k] for k in range(slots)]
    times = [start - WIN // 2 + ((at - start + WIN // 2) & (LANES - 1)) for start in starts]
    keys = [number * FAR + time for number, time in zip(numbers, times)]
    lane = lane_iota((1, LANES))

    sums = (jnp.zeros((HALF, LANES), jnp.float32),) * (slots * 2)
    def gather(j, sums, ks, load):
        sums = list(sums)
        for k in ks:
            number, start = table[j, 0, k], table[j, 1, k]
            piece = load(j, k, start)
            turned[j, k] = piece
            since = (lane - start) & (LANES - 1)
            spot = number * tiles + lax.shift_right_logical(since + start, 7)
            target[j, k : k + 1] = jnp.where(since < WIN, spot, -1)
            key = number * FAR + start
            for i in range(slots):
                since = keys[i] - key
                inside = (since >= 0) & (since < WIN)
                for h in range(2):
                    part = piece[h * HALF : (h + 1) * HALF]
                    sums[2 * i + h] = sums[2 * i + h] + jnp.where(inside, part, 0.0)
        return tuple(sums)

    def load_pair(j, k, start):
        return pltpu.roll(pieces_all[k // 2, j], (start + (k % 2) * WIN) & (LANES - 1), 1)

    def load_lone(j, k, start):
        upper = pltpu.roll(lone_all[j], start & (LANES - 1), 1)
        lower = pltpu.roll(lone_all[j], (start + WIN) & (LANES - 1), 1)
        return jnp.concatenate([upper, lower], axis=0)

    for g in range(slots // 2):
        settle(pieces_all.at[g], piece_recv.at[g])
        sums = each(n, functools.partial(gather, ks=(2 * g, 2 * g + 1), load=load_pair), sums)
    if slots % 2:
        settle(lone_all, lone_recv)
        sums = each(n, functools.partial(gather, ks=(slots - 1,), load=load_lone), sums)

    derived = []
    for k in range(slots):
        value = jnp.concatenate([stencil(sums[2 * k]), stencil(sums[2 * k + 1])], axis=0)
        derived.append(pltpu.roll(value, (k * SPAN + EDGE - starts[k]) & (LANES - 1), 1))
    wide = lane_iota((SB, LANES))
    settle(cuts_all, cut_recv)
    spreads = []
    for k in range(slots):
        stripes = []
        for i in range(strips):
            owner = numbers[k] * SB // rows + i
            begin, last = k * SPAN, (k + 1) * SPAN - 1
            stripe = cuts_all[owner, begin // LANES].astype(jnp.float32)
            if last // LANES > begin // LANES:
                follow = cuts_all[owner, last // LANES].astype(jnp.float32)
                stripe = jnp.where(lane_iota((lines, LANES)) >= begin % LANES, stripe, follow)
            stripes.append(stripe)
        block = stripes[0] if strips == 1 else jnp.concatenate(stripes, axis=0)
        time = ((wide - k * SPAN) & (LANES - 1)) + (starts[k] - EDGE)
        keep = (time >= 0) & (time < samples) & (jnp.full((SB, LANES), count[0, 0]) > k)
        window = -stencil(jnp.where(keep, derived[k] - block, 0.0))
        turn = k * SPAN + EDGE
        window = jnp.where(left, ahead(window, turn), ahead(window, turn - WIN))
        spread = jnp.concatenate([window] * (SB * WIN // LANES), axis=1)
        spreads.append(jnp.where(mask, spread, 0.0).astype(jnp.bfloat16))
    part = None
    for k in range(slots):
        term = jnp.dot(spreads[k], turned_w[k], preferred_element_type=jnp.float32)
        part = term if part is None else part + term
    grad[...] = jnp.sum(part, axis=0, keepdims=True)
    for i in range(ns - 1):
        remote(grad, parts.at[layer], sent, grad_recv, "sen", peer(layer, ns, i))
    pltpu.make_async_copy(grad, parts.at[layer], grad_recv).start()

    home = me * rows // SB * tiles

    def fill(i, carry):
        wanted = home + i

        def add(j, sums):
            low, high = sums
            for k in range(slots):
                here = jnp.broadcast_to(target[j, k : k + 1], (HALF, LANES)) == wanted
                low = low + jnp.where(here, turned[j, k, 0:HALF], 0.0)
                high = high + jnp.where(here, turned[j, k, HALF:SB], 0.0)
            return low, high

        low, high = each(n, add, (jnp.zeros((HALF, LANES), jnp.float32),) * 2)
        line = i // tiles * SB
        column = pl.ds(pl.multiple_of(i % tiles * LANES, LANES), LANES)
        signals[pl.ds(pl.multiple_of(line, SB), HALF), column] = low
        signals[pl.ds(pl.multiple_of(line + HALF, HALF), HALF), column] = high
        return carry

    lax.fori_loop(0, per * tiles, fill, 0)

    for r in range(0, rows, HALF):
        line = r if rows >= SB else pl.multiple_of((me * rows + r) % SB // HALF * HALF, HALF)
        block = stencil_edges(signals[pl.ds(line, HALF)])
        if rows % HALF == 0:
            residual[0, r : r + HALF] = block - measured[0, r : r + HALF].astype(jnp.float32)
        else:
            which = jnp.full((rows, samples), (me * rows) % HALF)
            own = block[0:rows]
            for i in range(1, HALF // rows):
                own = jnp.where(which == i * rows, block[i * rows : (i + 1) * rows], own)
            residual[0] = own - measured[0].astype(jnp.float32)

    settle(halo, halo_recv)
    tv = variation(n, me, image, halo)
    settle(table.at[pl.ds(0, n - 1)], sent)
    settle(halo, sent)
    settle(pieces_all.at[:, pl.ds(0, n - 1)], sent)
    if slots % 2:
        settle(lone_all.at[pl.ds(0, n - 1)], sent)
    settle(cuts_all.at[pl.ds(0, n - 1)], sent)
    settle(parts, grad_recv)
    flat = parts[0]
    for index in range(1, ns):
        flat = flat + parts[index]
    volume = image[0]
    width = volume.shape[1]
    for r in range(volume.shape[0]):
        total = flat[:, r * width : (r + 1) * width]
        out[0, r : r + 1] = volume[r : r + 1] - STEP_SIZE * (total + TV_WEIGHT * tv[r : r + 1])
    settle(parts.at[pl.ds(0, ns - 1)], sent)


def store_kernel(image, residual, image_out, residual_out, sem):
    rows = residual.shape[1]
    depth = rows // STORES if rows % (STORES * HALF) == 0 else rows
    copies = [pltpu.make_async_copy(image, image_out, sem.at[0])]
    for i, r in enumerate(range(0, rows, depth)):
        part = pl.ds(r, depth)
        copies.append(pltpu.make_async_copy(residual.at[:, part], residual_out.at[:, part], sem.at[1 + i]))
    for copy in copies:
        copy.start()
    for copy in copies:
        copy.wait()


def on_device(image, weights, block_ids, offsets, counts, measured):
    n = lax.axis_size("vox")
    ns = lax.axis_size("sen")
    slots, voxels, cells = weights.shape[2:]
    rows, samples = measured.shape[1:]
    pairs = slots // 2
    lines = min(rows, SB)
    chunks = (1,) * (slots - 1) + (2,)
    vmem = pl.BlockSpec(memory_space=pltpu.VMEM)
    hbm = pl.BlockSpec(memory_space=pltpu.HBM)
    smem = pl.BlockSpec(memory_space=pltpu.SMEM)
    dma = pltpu.SemaphoreType.DMA
    shape = jax.ShapeDtypeStruct

    def pin(value):
        return pltpu.with_memory_space_constraint(value, pltpu.HBM)

    image_next, residual = pl.pallas_call(
        functools.partial(step_kernel, n, ns, slots, chunks),
        out_shape=(shape(image.shape, jnp.float32), shape(measured.shape, jnp.float32)),
        in_specs=[hbm] * 4 + [smem, hbm],
        out_specs=(vmem, vmem),
        scratch_shapes=[
            pltpu.VMEM((slots, voxels, cells), jnp.bfloat16),
            pltpu.VMEM((slots, cells, voxels), jnp.bfloat16),
            pltpu.VMEM(image.shape, jnp.float32),
            pltpu.VMEM(measured.shape, measured.dtype),
            pltpu.VMEM((max(rows // SB, 1) * (samples // LANES), lines, LANES), jnp.bfloat16),
            pltpu.VMEM(block_ids.shape, jnp.int32),
            pltpu.VMEM(offsets.shape, jnp.int32),
            pltpu.VMEM((2, LANES), jnp.int32),
            pltpu.SMEM((n, 2, LANES), jnp.int32),
            pltpu.VMEM((2,) + image.shape[1:], jnp.float32),
            pltpu.VMEM((pairs, SB, LANES), jnp.float32),
            pltpu.VMEM((pairs, n, SB, LANES), jnp.float32),
            pltpu.VMEM((HALF, LANES), jnp.float32),
            pltpu.VMEM((n, HALF, LANES), jnp.float32),
            pltpu.VMEM((n, pl.cdiv(slots * SPAN, LANES), lines, LANES), jnp.bfloat16),
            pltpu.VMEM((n, pl.cdiv(slots * SPAN, LANES), lines, LANES), jnp.bfloat16),
            pltpu.VMEM((n, slots, SB, LANES), jnp.float32),
            pltpu.VMEM((n, HALF, LANES), jnp.int32),
            pltpu.VMEM((max(rows, SB), samples), jnp.float32),
            pltpu.VMEM((1, voxels), jnp.float32),
            pltpu.VMEM((ns, 1, voxels), jnp.float32),
            dma((sum(chunks),)),
            dma((2,)),
            dma,
            dma,
            dma,
            dma((pairs,)),
            dma,
            dma,
            dma,
        ],
        compiler_params=pltpu.CompilerParams(
            collective_id=0, has_side_effects=True, vmem_limit_bytes=40 << 20
        ),
        name="step_kernel",
    )(pin(image), pin(weights), pin(block_ids), pin(offsets), counts, pin(measured))

    return pl.pallas_call(
        store_kernel,
        out_shape=(shape(image.shape, jnp.float32), shape(measured.shape, jnp.float32)),
        in_specs=[vmem, vmem],
        out_specs=(hbm, hbm),
        scratch_shapes=[dma((1 + STORES,))],
        compiler_params=pltpu.CompilerParams(vmem_limit_bytes=1 << 20),
        name="store_kernel",
    )(image_next, residual)


def solution(mesh):
    placed = (
        P("vox", None, None),
        P("vox", "sen", None, None, None),
        P("vox", "sen", None),
        P("vox", "sen", None),
        P("vox", "sen"),
        P("sen", "vox", None),
    )
    return jax.shard_map(
        on_device,
        mesh=mesh,
        in_specs=placed,
        out_specs=(P("vox", None, None), P("sen", "vox", None)),
        check_vma=False,
    )
```
